256 devices in a mesh: band: 64 (over x, z, y_hi), img: 4 (over y_lo, core).
Axes of the slice: x: 4, y: 4 (y_hi: 2, y_lo: 2; y = y_hi * 2 + y_lo), z: 8, core: 2. Of those that a mesh axis runs over, the one named last changes fastest.
Arguments:
- pixels: bfloat16 [2048, 256, 180], P(('img', 'band')), parts along dimension 0, may hold values from -12 to 12
- keep_mask: int32 [256, 32], P(('img', 'band')), parts along dimension 0, may hold values from 0 to 1, as said below
- band_counts: int32 [256], P(('img', 'band')), parts along dimension 0, may hold values from 0 to 32, as said below
- plan_dest: int32 [256, 16], P(('img', 'band')), parts along dimension 0, may hold values from 0 to 63, as said below
- plan_slot: int32 [256, 16], P(('img', 'band')), parts along dimension 0, may hold values from 0 to 8, as said below
- bias_table: float32 [225, 6], replicated, may hold values from -4 to 4
- gain_attn: float32 [180], replicated, may hold values from 0.25 to 1.75
- qkv_weight: bfloat16 [180, 540], replicated, may hold values from -5 to 5
- proj_weight: bfloat16 [180, 180], replicated, may hold values from -0.4375 to 0.4375
- gain_mlp: float32 [180], replicated, may hold values from 0.25 to 1.75
- hidden_weight: bfloat16 [180, 360], replicated, may hold values from -0.4375 to 0.4375
- output_weight: bfloat16 [360, 180], replicated, may hold values from -0.3125 to 0.3125
Outputs:
- restored: bfloat16 [2048, 256, 180], P(('img', 'band')), parts along dimension 0
- work_tiles: bfloat16 [2048, 128, 180], P(('img', 'band')), parts along dimension 0
The draws below stay inside these ranges and needn't reach their ends.
There are 4 independent parts, one for each index of `img`. The reference program is written for one: setup_inputs(seed, part) draws one part's arguments, and reference() takes and returns one part's arrays. A program takes and returns all parts, laid end to end along the dimension named above; an argument that names none is the same for every part. Nothing has to cross between parts.
Inputs may be any that keep to these rules, and one draw needn't show every extreme that they name: `keep_mask`: the number of ones in a band varies strongly from band to band. band_counts[b] equals the number of ones among band b's windows in keep_mask. A band's live tiles are those with 2 t < band_counts[b]; their number summed over bands lies between 449 and 512, and some band has all 16 tiles live. `plan_dest`: within each aligned group of 64 consecutive tiles of a band (equal t // 64) the destinations are all different. `plan_slot`: 8 for tiles that are not live; a live tile has a slot below 8, no two live tiles of the image share destination and slot, and some destination receives 8 live tiles.
All inputs are finite; a program needn't handle non-finite values.
Results may differ from the reference program's by a relative error of at most 0.0044.
Values may be sent and summed in bfloat16 or wider, within the bound.
A program may use at most 64 MiB of HBM per device.

```python
import math
import jax
import jax.numpy as jnp
from jax import lax

CHAN = 180
HEADS = 6
FF_WIDTH = 360
WIN = 8
TILE = 2
ROWS = 8
WIDTH = 256
SHIFT = 4
TABLE = 225
HEIGHT = 512
WIN_DEV = 32
TILES_DEV = 16
CAP = 8
N_BAND = 64


def shuffle_band(band_key):
    return jax.random.permutation(band_key, WIN_DEV)


def plan_tables(key):
    key_perm = jax.random.fold_in(key, 101)
    key_share = jax.random.fold_in(key, 102)
    key_cut = jax.random.fold_in(key, 103)
    key_rest = jax.random.fold_in(key, 104)
    key_rank = jax.random.fold_in(key, 105)
    key_turn = jax.random.fold_in(key, 106)
    half_bands = N_BAND // 2
    band_order = jax.random.permutation(key_perm, N_BAND)
    shares = jax.random.randint(key_share, (half_bands,), 1, TILES_DEV + 1).astype(jnp.int32)
    shares = shares.at[0].set(TILES_DEV)
    trimmed = jax.random.randint(key_cut, (), 0, half_bands)
    pair_ids = jnp.arange(half_bands, dtype=jnp.int32)
    lowered = shares - ((pair_ids >= 1) & (pair_ids <= trimmed)).astype(jnp.int32)
    live_tiles = jnp.zeros((N_BAND,), jnp.int32).at[band_order[0::2]].set(lowered).at[band_order[1::2]].set(TILES_DEV - shares)
    spare_windows = jax.random.randint(key_rest, (N_BAND,), 0, TILE).astype(jnp.int32)
    kept_windows = jnp.where(live_tiles > 0, live_tiles * TILE - spare_windows, 0).astype(jnp.int32)
    window_ranks = jax.vmap(shuffle_band)(jax.random.split(key_rank, N_BAND))
    keep_table = (window_ranks < kept_windows[:, None]).astype(jnp.int32).reshape(HEIGHT // WIN, WIDTH // WIN)
    offsets = (jnp.cumsum(live_tiles) - live_tiles).astype(jnp.int32)
    rotation = jax.random.randint(key_turn, (), 0, N_BAND).astype(jnp.int32)
    tile_ids = jnp.arange(TILES_DEV, dtype=jnp.int32)
    global_tile = offsets[:, None] + tile_ids[None, :]
    dest_table = ((global_tile + rotation) % N_BAND).astype(jnp.int32)
    slot_table = jnp.where(tile_ids[None, :] < live_tiles[:, None], global_tile // N_BAND, CAP).astype(jnp.int32)
    return (keep_table, kept_windows, dest_table, slot_table)


def draw_keep_mask(key, part):
    return plan_tables(key)[0]


def draw_band_counts(key, part):
    return plan_tables(key)[1]


def draw_plan_dest(key, part):
    return plan_tables(key)[2]


def draw_plan_slot(key, part):
    return plan_tables(key)[3]


def draw_pixels(key, part):
    base_key = jax.random.fold_in(key, 201)
    values = jnp.clip(jax.random.normal(base_key, (HEIGHT, WIDTH, CHAN), jnp.float32), -6.0, 6.0)
    return values.astype(jnp.bfloat16)


def draw_qkv_weight(key, part):
    main_key = jax.random.fold_in(key, 301)
    weight = jax.random.normal(main_key, (CHAN, 3 * CHAN), jnp.float32) / math.sqrt(CHAN)
    return jnp.clip(weight, -5.0, 5.0).astype(jnp.bfloat16)


def noise(stream_key, shape, width, reach, kind=jnp.bfloat16):
    values = width * jax.random.normal(stream_key, shape, jnp.float32)
    return jnp.clip(values, min=-reach, max=reach).astype(kind)


def setup_inputs(seed: int = 0, part: int = 0) -> dict:
    seeds = jax.random.split(jax.random.key(seed), 13)
    part_keys = jax.random.split(jax.random.fold_in(seeds[12], part), 13)
    return {
        "pixels": draw_pixels(jax.random.fold_in(jax.random.fold_in(seeds[12], part), 71), part),
        "keep_mask": draw_keep_mask(jax.random.fold_in(jax.random.fold_in(seeds[12], part), 71), part),
        "band_counts": draw_band_counts(jax.random.fold_in(jax.random.fold_in(seeds[12], part), 71), part),
        "plan_dest": draw_plan_dest(jax.random.fold_in(jax.random.fold_in(seeds[12], part), 71), part),
        "plan_slot": draw_plan_slot(jax.random.fold_in(jax.random.fold_in(seeds[12], part), 71), part),
        "bias_table": noise(seeds[5], (TABLE, HEADS), 1.0, 4.0, jnp.float32),
        "gain_attn": jnp.clip(1.0 + 0.15 * jax.random.normal(seeds[6], (CHAN,), jnp.float32), 0.25, 1.75),
        "qkv_weight": draw_qkv_weight(jax.random.fold_in(seeds[12], 71), part),
        "proj_weight": noise(seeds[8], (CHAN, CHAN), CHAN ** -0.5, 0.4375),
        "gain_mlp": jnp.clip(1.0 + 0.15 * jax.random.normal(seeds[9], (CHAN,), jnp.float32), 0.25, 1.75),
        "hidden_weight": noise(seeds[10], (CHAN, FF_WIDTH), CHAN ** -0.5, 0.4375),
        "output_weight": noise(seeds[11], (FF_WIDTH, CHAN), FF_WIDTH ** -0.5, 0.3125),
    }


EPSILON = 1e-05

def layer_norm(values, gain_vec):
    values = values.astype(jnp.float32)
    center = values - lax.optimization_barrier(jnp.mean(values, axis=-1, keepdims=True))
    spread = lax.optimization_barrier(jnp.mean(center * center, axis=-1, keepdims=True))
    return center * lax.rsqrt(spread + EPSILON) * gain_vec

def position_bias(bias_table):
    coords = jnp.arange(WIN * WIN, dtype=jnp.int32)
    row_pos = coords // WIN
    col_pos = coords % WIN
    table_index = (row_pos[:, None] - row_pos[None, :] + WIN - 1) * (2 * WIN - 1) + (col_pos[:, None] - col_pos[None, :] + WIN - 1)
    return jnp.transpose(bias_table[table_index], (2, 0, 1))

def region_codes(first_row, row_count, height, col_count):
    rows_global = first_row + jnp.arange(row_count, dtype=jnp.int32)
    row_region = (rows_global >= height - WIN).astype(jnp.int32) + (rows_global >= height - SHIFT).astype(jnp.int32)
    col_global = jnp.arange(col_count, dtype=jnp.int32)
    col_region = (col_global >= col_count - WIN).astype(jnp.int32) + (col_global >= col_count - SHIFT).astype(jnp.int32)
    return 3 * row_region[:, None] + col_region[None, :]

def attend(windows, window_codes, head_bias, gain_attn, qkv_weight, proj_weight):
    window_count = windows.shape[0]
    head_dim = CHAN // HEADS
    normed = layer_norm(windows, gain_attn).astype(jnp.bfloat16).reshape(-1, CHAN)
    mixed_all = jnp.dot(normed, qkv_weight, preferred_element_type=jnp.float32).reshape(window_count, WIN * WIN, 3, HEADS, head_dim)
    queries = mixed_all[:, :, 0] * head_dim ** (-0.5)
    key_part = mixed_all[:, :, 1]
    value_part = lax.optimization_barrier(mixed_all[:, :, 2].astype(jnp.bfloat16)).astype(jnp.float32)
    scores = jnp.einsum('wqhd,wkhd->whqk', queries, key_part, precision=lax.Precision.HIGHEST)
    differ = window_codes[:, :, None] != window_codes[:, None, :]
    scores = scores + head_bias[None] + jnp.where(differ, -100.0, 0.0)[:, None]
    weights = jax.nn.softmax(scores, axis=-1).astype(jnp.bfloat16)
    weights = lax.optimization_barrier(weights).astype(jnp.float32)
    mixed = jnp.einsum('whqk,wkhd->wqhd', weights, value_part, precision=lax.Precision.HIGHEST)
    mixed = mixed.reshape(-1, CHAN).astype(jnp.bfloat16)
    projected = jnp.dot(mixed, proj_weight, preferred_element_type=jnp.float32)
    summed = windows.reshape(-1, CHAN).astype(jnp.float32) + projected
    return summed.astype(jnp.bfloat16).reshape(window_count, WIN * WIN, CHAN)

def feed(states, gain_mlp, hidden_weight, output_weight):
    flat_rows = states.reshape(-1, CHAN)
    normed = layer_norm(flat_rows, gain_mlp).astype(jnp.bfloat16)
    inner_act = jax.nn.gelu(jnp.dot(normed, hidden_weight, preferred_element_type=jnp.float32)).astype(jnp.bfloat16)
    summed = flat_rows.astype(jnp.float32) + jnp.dot(inner_act, output_weight, preferred_element_type=jnp.float32)
    return summed.astype(jnp.bfloat16).reshape(states.shape)

def reference(pixels, keep_mask, band_counts, plan_dest, plan_slot, bias_table, gain_attn, qkv_weight, proj_weight, gain_mlp, hidden_weight, output_weight):
    height = ROWS * N_BAND
    win_rows = ROWS // WIN
    win_cols = WIDTH // WIN
    shifted = jnp.roll(pixels, (-SHIFT, -SHIFT), axis=(0, 1))
    windows = shifted.reshape(N_BAND, win_rows, WIN, win_cols, WIN, CHAN).transpose(0, 1, 3, 2, 4, 5).reshape(N_BAND, WIN_DEV, WIN * WIN, CHAN)
    region_map = region_codes(0, height, height, WIDTH)
    window_codes = region_map.reshape(N_BAND, win_rows, WIN, win_cols, WIN).transpose(0, 1, 3, 2, 4).reshape(N_BAND, WIN_DEV, WIN * WIN)
    keep_rows = keep_mask.reshape(N_BAND, WIN_DEV)
    head_bias = position_bias(bias_table)

    def one_band(band_inputs):
        band_windows, band_codes, band_keep, band_count = band_inputs
        packed_order = (jnp.cumsum(band_keep) - 1).astype(jnp.int32)
        active = (band_keep == 1) & (packed_order < band_count)
        target = jnp.where(active, packed_order, WIN_DEV).astype(jnp.int32)
        packed = jnp.zeros((WIN_DEV + 1, WIN * WIN, CHAN), jnp.bfloat16).at[target].set(band_windows)[:WIN_DEV]
        packed_codes = jnp.zeros((WIN_DEV + 1, WIN * WIN), jnp.int32).at[target].set(band_codes)[:WIN_DEV]
        attended = attend(packed, packed_codes, head_bias, gain_attn, qkv_weight, proj_weight)
        finished = feed(attended, gain_mlp, hidden_weight, output_weight)
        unpacked = finished[jnp.clip(packed_order, 0, WIN_DEV - 1)]
        result = jnp.where(active[:, None, None], unpacked, band_windows)
        return (result, attended.reshape(TILES_DEV, TILE * WIN * WIN, CHAN))
    results, attended_all = lax.map(one_band, (windows, window_codes, keep_rows, band_counts))
    updated = results.reshape(N_BAND, win_rows, win_cols, WIN, WIN, CHAN).transpose(0, 1, 3, 2, 4, 5).reshape(height, WIDTH, CHAN)
    restored = jnp.roll(updated, (SHIFT, SHIFT), axis=(0, 1))
    tile_ids = jnp.arange(TILES_DEV, dtype=jnp.int32)
    tile_live = (tile_ids[None, :] * TILE < band_counts[:, None]) & (plan_slot < CAP)
    target = jnp.where(tile_live, plan_dest * CAP + plan_slot, N_BAND * CAP).astype(jnp.int32).reshape(-1)
    work_tiles = jnp.zeros((N_BAND * CAP + 1, TILE * WIN * WIN, CHAN), jnp.bfloat16)
    work_tiles = work_tiles.at[target].set(attended_all.reshape(-1, TILE * WIN * WIN, CHAN))[:N_BAND * CAP]
    return (restored, work_tiles)
```

```python
import functools

import jax
import jax.numpy as jnp
from jax import lax
from jax.experimental import pallas as pl
from jax.experimental.pallas import tpu as pltpu
from jax.sharding import PartitionSpec as P

CHAN = 180
HEADS = 6
HEAD_DIM = CHAN // HEADS
HEAD_PAD = 32
WIN = 8
TOKENS = WIN * WIN
TILE = 2
LANES = TILE * TOKENS
SHIFT = 4
CAP = 8
EPSILON = 1e-05
VMEM_LIMIT = 60 << 20


def from_behind(value, axis, steps):
    count = lax.axis_size(axis)
    pairs = [(source, (source + steps) % count) for source in range(count)]
    return lax.ppermute(value, axis, pairs)


def position_bias(bias_table):
    coords = jnp.arange(TOKENS, dtype=jnp.int32)
    row_pos = coords // WIN
    col_pos = coords % WIN
    table_index = (row_pos[None, :] - row_pos[:, None] + WIN - 1) * (2 * WIN - 1) + (
        col_pos[None, :] - col_pos[:, None] + WIN - 1
    )
    entries = bias_table.shape[0]
    onehot = (table_index.reshape(1, -1) == jnp.arange(entries, dtype=jnp.int32)[:, None]).astype(
        jnp.float32
    )
    looked = lax.dot_general(
        bias_table, onehot, (((0,), (0,)), ((), ())), precision=lax.Precision.HIGHEST
    )
    looked = looked.reshape(-1, TOKENS, TOKENS)
    return jnp.concatenate([looked, looked], axis=2)


def norm_columns(values, gain):
    center = values - jnp.sum(values, axis=0, keepdims=True) * (1.0 / CHAN)
    spread = jnp.sum(center * center, axis=0, keepdims=True) * (1.0 / CHAN)
    return (center * lax.rsqrt(spread + EPSILON) * gain).astype(jnp.bfloat16)


def split_two(values):
    high = values.astype(jnp.bfloat16)
    low = (values - high.astype(jnp.float32)).astype(jnp.bfloat16)
    return high, low


def attend_tile(x_cols, mask, gain, qkv_t, proj_t, bias_ref):
    lane = lax.broadcasted_iota(jnp.int32, (TOKENS, LANES), 1)
    first = lane < TOKENS
    normed = norm_columns(x_cols, gain)
    qkv = jnp.dot(qkv_t, normed, preferred_element_type=jnp.float32)
    mixed = []
    width = HEADS * HEAD_PAD
    for head in range(HEADS):
        at = head * HEAD_PAD
        query = qkv[at : at + HEAD_PAD] * HEAD_DIM ** (-0.5)
        key = qkv[width + at : width + at + HEAD_PAD]
        value = qkv[2 * width + at : 2 * width + at + HEAD_PAD].astype(jnp.bfloat16)
        query_high, query_low = split_two(query)
        key_high, key_low = split_two(key)
        left = jnp.concatenate([key_high, key_low, key_high], axis=0)
        right = jnp.concatenate([query_high, query_high, query_low], axis=0)
        full = lax.dot_general(
            left, right, (((0,), (0,)), ((), ())), preferred_element_type=jnp.float32
        )
        scores = jnp.where(first, full[:TOKENS], full[TOKENS:])
        scores = (scores + bias_ref[head]) + mask
        top = jnp.max(scores, axis=0, keepdims=True)
        grown = jnp.exp(scores - top)
        total = jnp.sum(grown, axis=0, keepdims=True)
        weights = grown * (1.0 / total)
        spread = jnp.concatenate(
            [jnp.where(first, weights, 0.0), jnp.where(first, 0.0, weights)], axis=0
        ).astype(jnp.bfloat16)
        mixed.append(jnp.dot(value, spread, preferred_element_type=jnp.float32).astype(jnp.bfloat16))
    mixed = jnp.concatenate(mixed, axis=0)
    projected = jnp.dot(proj_t, mixed, preferred_element_type=jnp.float32)
    return (x_cols + projected).astype(jnp.bfloat16)


def feed_tile(state, gain, hidden_t, output_t):
    state = state.astype(jnp.float32)
    normed = norm_columns(state, gain)
    hidden = jnp.dot(hidden_t, normed, preferred_element_type=jnp.float32)
    inner = jax.nn.gelu(hidden).astype(jnp.bfloat16)
    return state + jnp.dot(output_t, inner, preferred_element_type=jnp.float32)


def load_windows(pixels_ref, halo_ref, windows):
    count = windows.shape[0]

    def one(ref, source, row):
        values = ref[source].astype(jnp.float32)
        values = jnp.concatenate([values[SHIFT:], values[:SHIFT]], axis=0)
        windows[:, pl.ds(pl.multiple_of(row * WIN, WIN), WIN), :] = values.reshape(count, WIN, CHAN)

    for row in range(WIN - SHIFT):
        one(pixels_ref, row + SHIFT, row)
    for row in range(SHIFT):
        one(halo_ref, row, row + WIN - SHIFT)


def order_windows(keep_ref, count_ref, order):
    total = order.shape[0] - 1
    for place in range(total + 1):
        order[place] = total

    def step(index, position):
        kept = keep_ref[index]
        live = jnp.logical_and(kept == 1, position < count_ref[0])
        order[jnp.where(live, position, total)] = index
        return position + kept

    lax.fori_loop(0, total, step, jnp.int32(0))
    order[total] = total


def region_mask(last_band, last_first, last_second):
    key = lax.broadcasted_iota(jnp.int32, (TOKENS, LANES), 0)
    lane = lax.broadcasted_iota(jnp.int32, (TOKENS, LANES), 1)
    query = lane & (TOKENS - 1)
    rows_differ = ((key ^ query) & (SHIFT * WIN)) != 0
    cols_differ = ((key ^ query) & SHIFT) != 0
    last_col = jnp.where(lane < TOKENS, last_first, last_second)
    row_part = jnp.where(rows_differ, last_band, 0)
    col_part = jnp.where(cols_differ, last_col, 0)
    return jnp.where((row_part | col_part) != 0, -100.0, 0.0)


def attend_kernel(
    keep_ref, count_ref, band_ref, pixels_ref, halo_ref, gain_ref, qkv_ref, proj_ref, bias_ref, out_ref, windows, order
):
    total = windows.shape[0] - 1
    load_windows(pixels_ref, halo_ref, windows.at[pl.ds(0, total)])
    windows[total] = jnp.zeros((TOKENS, CHAN), jnp.float32)
    order_windows(keep_ref, count_ref, order)

    def step(tile, carry):
        one = order[tile * TILE]
        two = order[tile * TILE + 1]
        x_cols = jnp.concatenate([windows[one], windows[two]], axis=0).T
        mask = region_mask(
            band_ref[0], (one == total - 1).astype(jnp.int32), (two == total - 1).astype(jnp.int32)
        )
        out_ref[tile] = attend_tile(x_cols, mask, gain_ref[...], qkv_ref[...], proj_ref[...], bias_ref)
        return carry

    lax.fori_loop(0, out_ref.shape[0], step, 0, unroll=2)


def feed_kernel(
    keep_ref, count_ref, pixels_ref, halo_ref, state_ref, gain_ref, hidden_ref, output_ref, own_ref, sent_ref, windows, order
):
    total = windows.shape[0] - 1
    load_windows(pixels_ref, halo_ref, windows.at[pl.ds(0, total)])
    order_windows(keep_ref, count_ref, order)

    def step(tile, carry):
        done = feed_tile(state_ref[tile], gain_ref[...], hidden_ref[...], output_ref[...]).T
        windows[order[tile * TILE]] = done[:TOKENS]
        windows[order[tile * TILE + 1]] = done[TOKENS:]
        return carry

    lax.fori_loop(0, state_ref.shape[0], step, 0, unroll=2)
    for row in range(WIN):
        values = windows[0:total, row * WIN : (row + 1) * WIN, :].reshape(total * WIN, CHAN)
        values = jnp.concatenate([values[-SHIFT:], values[:-SHIFT]], axis=0).astype(jnp.bfloat16)
        if row < WIN - SHIFT:
            own_ref[row] = values
        else:
            sent_ref[row - WIN + SHIFT] = values


def pad_heads(weight):
    groups = weight.reshape(weight.shape[0], -1, HEAD_DIM)
    groups = jnp.pad(groups, ((0, 0), (0, 0), (0, HEAD_PAD - HEAD_DIM)))
    return groups.reshape(weight.shape[0], -1)


SMEM = pl.BlockSpec(memory_space=pltpu.SMEM)
VMEM = pl.BlockSpec(memory_space=pltpu.VMEM)


def shards(
    pixels,
    keep_mask,
    band_counts,
    plan_dest,
    plan_slot,
    bias_table,
    gain_attn,
    qkv_weight,
    proj_weight,
    gain_mlp,
    hidden_weight,
    output_weight,
):
    band_total = lax.axis_size("band")
    band_index = lax.axis_index("band")
    row_count, col_count, channels = pixels.shape
    window_total = keep_mask.shape[1]
    tile_total = window_total // TILE
    tile_tokens = TILE * TOKENS
    halo = from_behind(pixels[:SHIFT], "band", -1)
    last_band = (band_index == band_total - 1).astype(jnp.int32).reshape(1)
    keep = keep_mask.reshape(window_total)
    kept_count = band_counts[0]
    attended = pl.pallas_call(
        attend_kernel,
        out_shape=jax.ShapeDtypeStruct((tile_total, CHAN, LANES), jnp.bfloat16),
        in_specs=[SMEM] * 3 + [VMEM] * 6,
        out_specs=VMEM,
        scratch_shapes=[
            pltpu.VMEM((window_total + 1, TOKENS, CHAN), jnp.float32),
            pltpu.SMEM((window_total + 1,), jnp.int32),
        ],
        compiler_params=pltpu.CompilerParams(vmem_limit_bytes=VMEM_LIMIT),
        cost_estimate=pl.CostEstimate(flops=2 * 10**9, bytes_accessed=2 * 10**6, transcendentals=10**6),
        name="attend",
    )(
        keep,
        band_counts,
        last_band,
        pixels,
        halo,
        gain_attn.reshape(CHAN, 1),
        pad_heads(qkv_weight).T,
        pad_heads(proj_weight.T),
        position_bias(bias_table),
    )
    tile_ids = jnp.arange(tile_total, dtype=jnp.int32)
    tile_live = tile_ids * TILE < kept_count
    destinations = plan_dest[0]
    sent_slot = jnp.where(tile_live, plan_slot[0], CAP).astype(jnp.bfloat16)
    outgoing_slots = jnp.full((band_total, 1), CAP, jnp.bfloat16).at[destinations, 0].set(sent_slot)
    outgoing = jnp.zeros((band_total, CHAN, LANES), jnp.bfloat16).at[destinations].set(attended)
    incoming = lax.all_to_all(outgoing, "band", split_axis=0, concat_axis=0, tiled=True)
    incoming_slots = lax.all_to_all(outgoing_slots, "band", split_axis=0, concat_axis=0, tiled=True)
    own, sent = pl.pallas_call(
        feed_kernel,
        out_shape=[
            jax.ShapeDtypeStruct((row_count - SHIFT, col_count, CHAN), jnp.bfloat16),
            jax.ShapeDtypeStruct((SHIFT, col_count, CHAN), jnp.bfloat16),
        ],
        in_specs=[SMEM] * 2 + [VMEM] * 6,
        out_specs=[VMEM, VMEM],
        scratch_shapes=[
            pltpu.VMEM((window_total + 1, TOKENS, CHAN), jnp.float32),
            pltpu.SMEM((window_total + 1,), jnp.int32),
        ],
        compiler_params=pltpu.CompilerParams(vmem_limit_bytes=VMEM_LIMIT),
        cost_estimate=pl.CostEstimate(flops=2 * 10**9, bytes_accessed=2 * 10**6, transcendentals=10**6),
        name="feed",
    )(
        keep,
        band_counts,
        pixels,
        halo,
        attended,
        gain_mlp.reshape(CHAN, 1),
        hidden_weight.T,
        output_weight.T,
    )
    arrived_slot = incoming_slots.reshape(-1).astype(jnp.int32)
    work = (
        jnp.zeros((CAP, CHAN, LANES), jnp.bfloat16).at[arrived_slot].set(incoming, mode="drop")
    )
    work = jnp.transpose(work, (0, 2, 1))
    upper_rows = from_behind(sent, "band", 1)
    restored = jnp.concatenate([upper_rows, own], axis=0)
    return (restored, work)


def solution(mesh):
    sharded = P(("img", "band"))
    in_specs = (
        P(("img", "band"), None, None),
        P(("img", "band"), None),
        sharded,
        P(("img", "band"), None),
        P(("img", "band"), None),
    ) + (P(),) * 7
    out_specs = (P(("img", "band"), None, None), P(("img", "band"), None, None))
    return jax.shard_map(shards, mesh=mesh, in_specs=in_specs, out_specs=out_specs, check_vma=False)
```

```python
import jax
import jax.numpy as jnp
from jax import lax
from jax.experimental import pallas as pl
from jax.experimental.pallas import tpu as pltpu
from jax.sharding import PartitionSpec as P

CHAN = 180
HEADS = 6
HEAD_DIM = CHAN // HEADS
HEAD_PAD = 32
WIN = 8
TOKENS = WIN * WIN
TILE = 2
LANES = TILE * TOKENS
SHIFT = 4
CAP = 8
ROWS_PAD = 184
X_SIZE = 4
Z_SIZE = 8
Y_SIZE = 2
EPSILON = 1e-05
MESH = pl.DeviceIdType.MESH
VMEM_LIMIT = 60 << 20


def from_behind(value, axis, steps):
    count = lax.axis_size(axis)
    pairs = [(source, (source + steps) % count) for source in range(count)]
    return lax.ppermute(value, axis, pairs)


def position_bias(bias_table):
    coords = jnp.arange(TOKENS, dtype=jnp.int32)
    row_pos = coords // WIN
    col_pos = coords % WIN
    table_index = (row_pos[None, :] - row_pos[:, None] + WIN - 1) * (2 * WIN - 1) + (
        col_pos[None, :] - col_pos[:, None] + WIN - 1
    )
    entries = bias_table.shape[0]
    onehot = (table_index.reshape(1, -1) == jnp.arange(entries, dtype=jnp.int32)[:, None]).astype(
        jnp.float32
    )
    looked = lax.dot_general(
        bias_table, onehot, (((0,), (0,)), ((), ())), precision=lax.Precision.HIGHEST
    )
    looked = looked.reshape(-1, TOKENS, TOKENS)
    return jnp.concatenate([looked, looked], axis=2)


def clear_pad(values):
    edge = CHAN - CHAN % 8
    row = lax.broadcasted_iota(jnp.int32, (ROWS_PAD - edge, LANES), 0)
    return jnp.concatenate([values[:edge], jnp.where(row < CHAN - edge, values[edge:], 0.0)], axis=0)


def norm_columns(values, gain):
    center = clear_pad(values - jnp.sum(values, axis=0, keepdims=True) * (1.0 / CHAN))
    spread = jnp.sum(center * center, axis=0, keepdims=True) * (1.0 / CHAN)
    return (center * lax.rsqrt(spread + EPSILON) * gain).astype(jnp.bfloat16)


def split_two(values):
    high = values.astype(jnp.bfloat16)
    low = (values - high.astype(jnp.float32)).astype(jnp.bfloat16)
    return high, low


def attend_tile(x_cols, mask, gain, qkv_t, proj_t, bias_ref):
    lane = lax.broadcasted_iota(jnp.int32, (TOKENS, LANES), 1)
    first = lane < TOKENS
    normed = norm_columns(x_cols, gain)
    qkv = jnp.dot(qkv_t, normed, preferred_element_type=jnp.float32)
    mixed = []
    width = HEADS * HEAD_PAD
    for head in range(HEADS):
        at = head * HEAD_PAD
        query = qkv[at : at + HEAD_PAD] * HEAD_DIM ** (-0.5)
        key = qkv[width + at : width + at + HEAD_PAD]
        value = qkv[2 * width + at : 2 * width + at + HEAD_PAD].astype(jnp.bfloat16)
        query_high, query_low = split_two(query)
        key_high, key_low = split_two(key)
        left = jnp.concatenate([key_high, key_low, key_high], axis=0)
        right = jnp.concatenate([query_high, query_high, query_low], axis=0)
        full = lax.dot_general(
            left, right, (((0,), (0,)), ((), ())), preferred_element_type=jnp.float32
        )
        scores = jnp.where(first, full[:TOKENS], full[TOKENS:])
        scores = (scores + bias_ref[head]) + mask
        top = jnp.max(scores, axis=0, keepdims=True)
        grown = jnp.exp(scores - top)
        total = jnp.sum(grown, axis=0, keepdims=True)
        weights = grown * (1.0 / total)
        spread = jnp.concatenate(
            [jnp.where(first, weights, 0.0), jnp.where(first, 0.0, weights)], axis=0
        ).astype(jnp.bfloat16)
        mixed.append(jnp.dot(value, spread, preferred_element_type=jnp.float32).astype(jnp.bfloat16))
    mixed = jnp.concatenate(mixed, axis=0)
    projected = jnp.dot(proj_t, mixed, preferred_element_type=jnp.float32)
    return x_cols + projected


def feed_tile(state, gain, hidden_t, output_t):
    state = clear_pad(state.astype(jnp.float32))
    normed = norm_columns(state, gain)
    hidden = jnp.dot(hidden_t, normed, preferred_element_type=jnp.float32)
    inner = jax.nn.gelu(hidden).astype(jnp.bfloat16)
    return state + jnp.dot(output_t, inner, preferred_element_type=jnp.float32)


def load_windows(pixels_ref, halo_ref, windows):
    count = windows.shape[0]

    def one(ref, source, row):
        values = ref[source].astype(jnp.float32)
        values = jnp.concatenate([values[SHIFT:], values[:SHIFT]], axis=0)
        values = values.reshape(count, WIN, CHAN)
        windows[:, pl.ds(pl.multiple_of(row * WIN, WIN), WIN), 0:CHAN] = values

    for row in range(WIN - SHIFT):
        one(pixels_ref, row + SHIFT, row)
    for row in range(SHIFT):
        one(halo_ref, row, row + WIN - SHIFT)


def order_windows(keep_ref, count_ref, order, source_ref):
    total = order.shape[0] - 1
    for place in range(total + 1):
        order[place] = total

    def step(index, position):
        kept = keep_ref[index]
        live = jnp.logical_and(kept == 1, position < count_ref[0])
        order[jnp.where(live, position, total)] = index
        source_ref[index] = jnp.where(live, position + total, index)
        return position + kept

    lax.fori_loop(0, total, step, jnp.int32(0))
    order[total] = total


def region_mask(last_band, last_first, last_second):
    key = lax.broadcasted_iota(jnp.int32, (TOKENS, LANES), 0)
    lane = lax.broadcasted_iota(jnp.int32, (TOKENS, LANES), 1)
    query = lane & (TOKENS - 1)
    rows_differ = ((key ^ query) & (SHIFT * WIN)) != 0
    cols_differ = ((key ^ query) & SHIFT) != 0
    last_col = jnp.where(lane < TOKENS, last_first, last_second)
    row_part = jnp.where(rows_differ, last_band, 0)
    col_part = jnp.where(cols_differ, last_col, 0)
    return jnp.where((row_part | col_part) != 0, -100.0, 0.0)


def attend_kernel(
    keep_ref,
    count_ref,
    dest_ref,
    slot_ref,
    band_ref,
    pixels_ref,
    halo_ref,
    gain_ref,
    qkv_ref,
    proj_ref,
    bias_ref,
    out_ref,
    held_ref,
    source_ref,
    windows,
    order,
):
    total = windows.shape[0] - 1
    tiles = out_ref.shape[0] - 1
    bands = held_ref.shape[0] - 1
    windows[:, :, CHAN:] = jnp.zeros((total + 1, TOKENS, ROWS_PAD - CHAN), jnp.float32)
    load_windows(pixels_ref, halo_ref, windows.at[pl.ds(0, total)])
    windows[total] = jnp.zeros((TOKENS, ROWS_PAD), jnp.float32)
    order_windows(keep_ref, count_ref, order, source_ref)
    for band in range(bands + 1):
        held_ref[band] = tiles
    row = lax.broadcasted_iota(jnp.int32, (ROWS_PAD, LANES), 0)

    def step(tile, carry):
        slot = slot_ref[tile]
        live = jnp.logical_and(tile * TILE < count_ref[0], slot < CAP)
        held_ref[jnp.where(live, dest_ref[tile], bands)] = tile
        one = order[tile * TILE]
        two = order[tile * TILE + 1]
        x_cols = jnp.concatenate([windows[one], windows[two]], axis=0).T
        mask = region_mask(
            band_ref[0], (one == total - 1).astype(jnp.int32), (two == total - 1).astype(jnp.int32)
        )
        done = attend_tile(x_cols, mask, gain_ref[...], qkv_ref[...], proj_ref[...], bias_ref)
        out_ref[tile] = jnp.where(row < CHAN, done, slot.astype(jnp.float32)).astype(jnp.bfloat16)
        return carry

    lax.fori_loop(0, tiles, step, 0, unroll=2)
    out_ref[tiles] = jnp.where(row < CHAN, 0.0, float(CAP)).astype(jnp.bfloat16)
    held_ref[bands] = tiles


def band_of(x, z, y):
    return (lax.rem(x, X_SIZE) * Z_SIZE + lax.rem(z, Z_SIZE)) * Y_SIZE + lax.rem(y, Y_SIZE)


def exchange_kernel(
    held_ref,
    source_ref,
    pixels_ref,
    halo_ref,
    state_ref,
    gain_ref,
    hidden_ref,
    output_ref,
    restored_ref,
    work_ref,
    pool,
    windows,
    sent_rows,
    got_rows,
    y_out,
    x_out,
    x_in,
    z_out,
    z_in,
    total_ref,
    rows_sem,
    y_sem,
    x_sem,
    z_sem,
):
    me = lax.axis_index("band")
    bands = lax.axis_size("band")
    x = me // (Z_SIZE * Y_SIZE)
    z = lax.rem(me // Y_SIZE, Z_SIZE)
    y = lax.rem(me, Y_SIZE)
    x_peers = [band_of(x + step, z, y) for step in range(1, X_SIZE)]
    y_peer = band_of(x, z, y + 1)
    z_peers = [band_of(x, z + 1, y), band_of(x, z + Z_SIZE - 1, y)]
    after = lax.rem(me + 1, bands)
    before = lax.rem(me + bands - 1, bands)
    barrier = pltpu.get_barrier_semaphore()
    greeted = x_peers + [y_peer] + z_peers + [after, before]
    for peer in greeted:
        pl.semaphore_signal(barrier, inc=1, device_id={"band": peer}, device_id_type=MESH)

    far = Z_SIZE // 2
    order = [far]
    for away in range(far - 1, 0, -1):
        order += [away, Z_SIZE - away]
    order += [0]

    def stage(away):
        def step(ahead, carry):
            y_out[away, ahead] = state_ref[held_ref[band_of(x + ahead, z + away, y + 1)]]
            x_out[away, 0, ahead] = state_ref[held_ref[band_of(x + ahead, z + away, y)]]
            return carry

        lax.fori_loop(0, X_SIZE, step, 0)

    def copy(source, target, sems, index, peer):
        return pltpu.make_async_remote_copy(
            src_ref=source,
            dst_ref=target,
            send_sem=sems.at[(0,) + index],
            recv_sem=sems.at[(1,) + index],
            device_id={"band": peer},
            device_id_type=MESH,
        )

    def y_copy(away):
        return copy(y_out.at[away], x_out.at[away, 1], y_sem, (away,), y_peer)

    def x_copy(away, ahead):
        return copy(
            x_out.at[away, :, ahead], x_in.at[away, ahead - 1], x_sem, (away, ahead - 1), x_peers[ahead - 1]
        )

    half = CAP // 2

    def z_copy(side, hop, part):
        piece = pl.ds(part * half, half)
        return copy(
            z_out.at[side, hop, piece], z_in.at[side, hop, piece], z_sem, (side, hop, part), z_peers[side]
        )

    def pass_x(away):
        y_copy(away).wait_recv()
        for ahead in range(1, X_SIZE):
            x_copy(away, ahead).start()

    def wait_x(away):
        for ahead in range(1, X_SIZE):
            x_copy(away, ahead).wait_recv()

    def gather(away, part, target, arrived):
        found = [x_out.at[away, 0, 0], x_out.at[away, 1, 0]]
        for ahead in range(X_SIZE - 1):
            found += [x_in.at[away, ahead, 0], x_in.at[away, ahead, 1]]

        def step(index, carry):
            slot = part * half + index
            number = slot.astype(jnp.float32)
            sum_ = None if arrived is None else arrived[slot]
            for one in found:
                mark = one[CHAN : CHAN + 1, :].astype(jnp.float32)
                term = one[...] * jnp.where(mark == number, 1.0, 0.0).astype(jnp.bfloat16)
                sum_ = term if sum_ is None else sum_ + term
            target[slot] = sum_
            return carry

        lax.fori_loop(0, half, step, 0)

    fed = [0]

    def feed(count):
        start = fed[0]

        def step(tile, carry):
            done = feed_tile(state_ref[tile], gain_ref[...], hidden_ref[...], output_ref[...]).T
            base = window_total + tile * TILE
            pool[base] = done[:TOKENS, :CHAN]
            pool[base + 1] = done[TOKENS:, :CHAN]
            return carry

        lax.fori_loop(start, start + count, step, 0, unroll=min(count, 2))
        fed[0] = start + count

    window_total = source_ref.shape[0]
    tiles = state_ref.shape[0] - 1
    share = tiles // 8

    for away in order:
        stage(away)
    pl.semaphore_wait(barrier, len(greeted))
    for away in order:
        y_copy(away).start()
    load_windows(pixels_ref, halo_ref, pool.at[pl.ds(0, window_total)])

    def hop_far():
        wait_x(far)
        for side in range(2):
            gather(far, side, z_out.at[side, 0], None)
            z_copy(side, 0, side).start()

    def hop(side, number):
        away = far - number if side == 0 else Z_SIZE - far + number
        wait_x(away)
        parts = (1 - side, side) if number == 1 else (0, 1)
        for part in parts:
            if number == 1 and part != side:
                arrived = None
            else:
                z_copy(side, number - 1, part).wait_recv()
                arrived = z_in.at[side, number - 1]
            gather(away, part, z_out.at[side, number], arrived)
            z_copy(side, number, part).start()

    def rows_copy():
        return copy(sent_rows, got_rows, rows_sem, (), after)

    def rows(first, count, target):
        for row in range(count):
            at = (first + row) * WIN
            values = windows[:, at : at + WIN, :].reshape(window_total * WIN, CHAN)
            values = jnp.concatenate([values[-SHIFT:], values[:-SHIFT]], axis=0)
            target[row] = values.astype(jnp.bfloat16)

    pass_x(order[0])
    feed(share)
    pass_x(order[1])
    pass_x(order[2])
    feed(share)
    hop_far()
    feed(share)
    pass_x(order[3])
    pass_x(order[4])
    feed(share)
    hop(0, 1)
    feed(share)
    hop(1, 1)
    pass_x(order[5])
    pass_x(order[6])
    feed(share)
    hop(0, 2)
    feed(share)
    hop(1, 2)
    pass_x(order[7])
    feed(tiles - fed[0])

    def move(window, carry):
        windows[window] = pool[source_ref[window]]
        return carry

    lax.fori_loop(0, window_total, move, 0)
    rows(WIN - SHIFT, SHIFT, sent_rows)
    rows_copy().start()
    hop(0, 3)
    hop(1, 3)
    rows(0, WIN - SHIFT, restored_ref.at[pl.ds(SHIFT, WIN - SHIFT)])
    wait_x(0)
    for part in range(2):
        gather(0, part, total_ref, None)
    rows_copy().wait_recv()
    restored_ref[0:SHIFT] = got_rows[...]
    for part in range(2):
        for side in range(2):
            z_copy(side, far - 1, part).wait_recv()

        def finish(index, carry):
            slot = part * half + index
            values = total_ref[slot] + z_in[0, far - 1, slot] + z_in[1, far - 1, slot]
            work_ref[slot] = values.astype(jnp.float32).T[:, :CHAN].astype(jnp.bfloat16)
            return carry

        lax.fori_loop(0, half, finish, 0)
    for away in order:
        y_copy(away).wait_send()
        for ahead in range(1, X_SIZE):
            x_copy(away, ahead).wait_send()
    for side in range(2):
        z_copy(side, 0, side).wait_send()
        for number in range(1, far):
            for part in range(2):
                z_copy(side, number, part).wait_send()
    rows_copy().wait_send()


def pad_heads(weight):
    groups = weight.reshape(weight.shape[0], -1, HEAD_DIM)
    groups = jnp.pad(groups, ((0, 0), (0, 0), (0, HEAD_PAD - HEAD_DIM)))
    return groups.reshape(weight.shape[0], -1)


SMEM = pl.BlockSpec(memory_space=pltpu.SMEM)
VMEM = pl.BlockSpec(memory_space=pltpu.VMEM)


def shards(
    pixels,
    keep_mask,
    band_counts,
    plan_dest,
    plan_slot,
    bias_table,
    gain_attn,
    qkv_weight,
    proj_weight,
    gain_mlp,
    hidden_weight,
    output_weight,
):
    band_total = lax.axis_size("band")
    band_index = lax.axis_index("band")
    row_count, col_count, channels = pixels.shape
    window_total = keep_mask.shape[1]
    tile_total = window_total // TILE
    halo = from_behind(pixels[:SHIFT], "band", -1)
    last_band = (band_index == band_total - 1).astype(jnp.int32).reshape(1)
    keep = keep_mask.reshape(window_total)
    pad = ROWS_PAD - CHAN
    tiles, held, source = pl.pallas_call(
        attend_kernel,
        out_shape=[
            jax.ShapeDtypeStruct((tile_total + 1, ROWS_PAD, LANES), jnp.bfloat16),
            jax.ShapeDtypeStruct((band_total + 1,), jnp.int32),
            jax.ShapeDtypeStruct((window_total,), jnp.int32),
        ],
        in_specs=[SMEM] * 5 + [VMEM] * 6,
        out_specs=[VMEM, SMEM, SMEM],
        scratch_shapes=[
            pltpu.VMEM((window_total + 1, TOKENS, ROWS_PAD), jnp.float32),
            pltpu.SMEM((window_total + 1,), jnp.int32),
        ],
        compiler_params=pltpu.CompilerParams(vmem_limit_bytes=VMEM_LIMIT),
        cost_estimate=pl.CostEstimate(flops=2 * 10**9, bytes_accessed=2 * 10**6, transcendentals=10**6),
        name="attend",
    )(
        keep,
        band_counts,
        plan_dest.reshape(-1),
        plan_slot.reshape(-1),
        last_band,
        pixels,
        halo,
        jnp.pad(gain_attn, (0, pad)).reshape(ROWS_PAD, 1),
        jnp.pad(pad_heads(qkv_weight), ((0, pad), (0, 0))).T,
        jnp.pad(pad_heads(proj_weight.T), ((0, pad), (0, 0))),
        position_bias(bias_table),
    )
    tile_shape = (ROWS_PAD, LANES)
    far = Z_SIZE // 2
    restored, work = pl.pallas_call(
        exchange_kernel,
        out_shape=[
            jax.ShapeDtypeStruct((row_count, col_count, CHAN), jnp.bfloat16),
            jax.ShapeDtypeStruct((CAP, LANES, CHAN), jnp.bfloat16),
        ],
        in_specs=[SMEM] * 2 + [VMEM] * 6,
        out_specs=[VMEM, VMEM],
        scratch_shapes=[
            pltpu.VMEM((2 * window_total, TOKENS, CHAN), jnp.float32),
            pltpu.VMEM((window_total, TOKENS, CHAN), jnp.float32),
            pltpu.VMEM((SHIFT, col_count, CHAN), jnp.bfloat16),
            pltpu.VMEM((SHIFT, col_count, CHAN), jnp.bfloat16),
            pltpu.VMEM((Z_SIZE, X_SIZE) + tile_shape, jnp.bfloat16),
            pltpu.VMEM((Z_SIZE, Y_SIZE, X_SIZE) + tile_shape, jnp.bfloat16),
            pltpu.VMEM((Z_SIZE, X_SIZE - 1, Y_SIZE) + tile_shape, jnp.bfloat16),
            pltpu.VMEM((2, far, CAP) + tile_shape, jnp.bfloat16),
            pltpu.VMEM((2, far, CAP) + tile_shape, jnp.bfloat16),
            pltpu.VMEM((CAP,) + tile_shape, jnp.bfloat16),
            pltpu.SemaphoreType.DMA((2,)),
            pltpu.SemaphoreType.DMA((2, Z_SIZE)),
            pltpu.SemaphoreType.DMA((2, Z_SIZE, X_SIZE - 1)),
            pltpu.SemaphoreType.DMA((2, 2, far, 2)),
        ],
        compiler_params=pltpu.CompilerParams(
            vmem_limit_bytes=VMEM_LIMIT, collective_id=0, has_side_effects=True
        ),
        cost_estimate=pl.CostEstimate(flops=2 * 10**9, bytes_accessed=2 * 10**6, transcendentals=10**6),
        name="exchange",
    )(
        held,
        source,
        pixels,
        halo,
        tiles,
        jnp.pad(gain_mlp, (0, pad)).reshape(ROWS_PAD, 1),
        jnp.pad(hidden_weight, ((0, pad), (0, 0))).T,
        jnp.pad(output_weight, ((0, 0), (0, pad))).T,
    )
    return (restored, work)


def solution(mesh):
    sharded = P(("img", "band"))
    in_specs = (
        P(("img", "band"), None, None),
        P(("img", "band"), None),
        sharded,
        P(("img", "band"), None),
        P(("img", "band"), None),
    ) + (P(),) * 7
    out_specs = (P(("img", "band"), None, None), P(("img", "band"), None, None))
    return jax.shard_map(shards, mesh=mesh, in_specs=in_specs, out_specs=out_specs, check_vma=False)
```

```python
import jax
import jax.numpy as jnp
from jax import lax
from jax.experimental import pallas as pl
from jax.experimental.pallas import tpu as pltpu
from jax.sharding import PartitionSpec as P

CHAN = 180
FF_WIDTH = 360
HEADS = 6
HEAD_DIM = CHAN // HEADS
HEAD_PAD = 32
WIN = 8
TOKENS = WIN * WIN
TILE = 2
LANES = TILE * TOKENS
SHIFT = 4
CAP = 8
ROWS_PAD = 184
X_SIZE = 4
Z_SIZE = 8
Y_SIZE = 2
EPSILON = 1e-05
MESH = pl.DeviceIdType.MESH
VMEM_LIMIT = 60 << 20


def norm_columns(values, gain):
    center = values - jnp.sum(values, axis=0, keepdims=True) * (1.0 / CHAN)
    spread = jnp.sum(center * center, axis=0, keepdims=True) * (1.0 / CHAN)
    return (center * lax.rsqrt(spread + EPSILON) * gain).astype(jnp.bfloat16)


def split_two(values):
    high = values.astype(jnp.bfloat16)
    low = (values - high.astype(jnp.float32)).astype(jnp.bfloat16)
    return high, low


def attend_tile(x_cols, mask, gain, qkv_t, proj_t, bias_ref):
    lane = lax.broadcasted_iota(jnp.int32, (TOKENS, LANES), 1)
    first = lane < TOKENS
    normed = norm_columns(x_cols, gain)
    qkv = jnp.dot(qkv_t, normed, preferred_element_type=jnp.float32)
    mixed = []
    width = HEADS * HEAD_PAD
    for head in range(HEADS):
        at = head * HEAD_PAD
        query = qkv[at : at + HEAD_PAD] * HEAD_DIM ** (-0.5)
        key = qkv[width + at : width + at + HEAD_PAD]
        value = qkv[2 * width + at : 2 * width + at + HEAD_PAD].astype(jnp.bfloat16)
        query_high, query_low = split_two(query)
        key_high, key_low = split_two(key)
        left = jnp.concatenate([key_high, key_low, key_high], axis=0)
        right = jnp.concatenate([query_high, query_high, query_low], axis=0)
        full = lax.dot_general(
            left, right, (((0,), (0,)), ((), ())), preferred_element_type=jnp.float32
        )
        scores = jnp.where(first, full[:TOKENS], full[TOKENS:])
        scores = (scores + bias_ref[head]) + mask
        top = jnp.max(scores, axis=0, keepdims=True)
        grown = jnp.exp(scores - top)
        total = jnp.sum(grown, axis=0, keepdims=True)
        weights = grown * (1.0 / total)
        spread = jnp.concatenate(
            [jnp.where(first, weights, 0.0), jnp.where(first, 0.0, weights)], axis=0
        ).astype(jnp.bfloat16)
        mixed.append(jnp.dot(value, spread, preferred_element_type=jnp.float32).astype(jnp.bfloat16))
    mixed = jnp.concatenate(mixed, axis=0)
    projected = jnp.dot(proj_t, mixed, preferred_element_type=jnp.float32)
    return (x_cols + projected).astype(jnp.bfloat16)


def feed_tile(state, gain, hidden_t, output_t):
    state = state.astype(jnp.float32)
    normed = norm_columns(state, gain)
    hidden = jnp.dot(hidden_t, normed, preferred_element_type=jnp.float32)
    inner = jax.nn.gelu(hidden).astype(jnp.bfloat16)
    return state + jnp.dot(output_t, inner, preferred_element_type=jnp.float32)


def iota(shape, dim):
    return lax.broadcasted_iota(jnp.int32, shape, dim)


def region_mask(rows_split, cols_split):
    key = iota((TOKENS, LANES), 0)
    query = iota((TOKENS, LANES), 1) & (TOKENS - 1)
    rows_differ = ((key ^ query) & (SHIFT * WIN)) != 0
    cols_differ = ((key ^ query) & SHIFT) != 0
    row_part = jnp.where(rows_differ, rows_split, 0)
    col_part = jnp.where(cols_differ, cols_split, 0)
    return jnp.where((row_part | col_part) != 0, -100.0, 0.0)


def head_columns(count):
    row = iota((count * HEAD_PAD, count * HEAD_DIM), 0)
    col = iota((count * HEAD_PAD, count * HEAD_DIM), 1)
    inside = row & (HEAD_PAD - 1)
    want = (row >> 5) * HEAD_DIM + inside
    hit = jnp.logical_and(inside < HEAD_DIM, col == want)
    return jnp.where(hit, 1.0, 0.0).astype(jnp.bfloat16)


def build_bias(table_ref, bias_ref):
    span = 2 * WIN - 1
    entries = table_ref.shape[1]
    entry = iota((entries, WIN * LANES), 0)
    lane = iota((entries, WIN * LANES), 1)
    key_col = lane >> 7
    place = lane & (LANES - 1)
    want = (place >> 3) * span + (place & (WIN - 1)) - key_col + WIN - 1
    onehot = jnp.where(entry == want, 1.0, 0.0)
    looked = jnp.dot(
        table_ref[...], onehot, precision=lax.Precision.HIGHEST, preferred_element_type=jnp.float32
    )
    low = iota((HEADS, LANES), 1) < TOKENS
    for col in range(WIN):
        line = looked[:, col * LANES : (col + 1) * LANES]
        for row in range(WIN):
            back = (WIN - 1 - row) * WIN
            moved = line if back == 0 else pltpu.roll(line, LANES - back, 1)
            moved = jnp.where(low, moved, pltpu.roll(moved, TOKENS, 1))
            bias_ref[:, row * WIN + col, :] = moved


def swap_blocks(blocks):
    lane = iota(blocks[0].shape, 1)
    blocks = list(blocks)
    for bit in range(3):
        width = 16 << bit
        low = (lane & width) == 0
        for one in range(8):
            if one & (1 << bit):
                continue
            two = one | (1 << bit)
            first, second = blocks[one], blocks[two]
            blocks[one] = jnp.where(low, first, pltpu.roll(second, width, 1))
            blocks[two] = jnp.where(low, pltpu.roll(first, LANES - width, 1), second)
    return blocks


def shift_lanes(first, second, steps):
    lane = iota(first.shape, 1)
    first, second = pltpu.roll(first, steps % LANES, 1), pltpu.roll(second, steps % LANES, 1)
    own = lane >= steps if steps > 0 else lane < LANES + steps
    return jnp.where(own, first, second), jnp.where(own, second, first)


def plan_kernel(keep_ref, count_ref, dest_ref, slot_ref, order_ref, held_ref, active_ref):
    total = active_ref.shape[0]
    bands = held_ref.shape[0] - 1
    tiles = dest_ref.shape[0]
    for place in range(total + 1):
        order_ref[place] = total
    for band in range(bands + 1):
        held_ref[band] = tiles

    def window_step(index, position):
        kept = keep_ref[index]
        live = jnp.logical_and(kept == 1, position < count_ref[0])
        order_ref[jnp.where(live, position, total)] = index
        active_ref[index] = live.astype(jnp.int32)
        return position + kept

    lax.fori_loop(0, total, window_step, jnp.int32(0))

    def tile_step(tile, carry):
        live = jnp.logical_and(tile * TILE < count_ref[0], slot_ref[tile] < CAP)
        held_ref[jnp.where(live, dest_ref[tile], bands)] = tile
        return carry

    lax.fori_loop(0, tiles, tile_step, 0)


def band_of(x, z, y):
    return (lax.rem(x, X_SIZE) * Z_SIZE + lax.rem(z, Z_SIZE)) * Y_SIZE + lax.rem(y, Y_SIZE)


UNITS = (2, 1, 1, 2, 2, 2, 2, 2, 2)


def block_kernel(
    held_ref,
    order_ref,
    active_ref,
    slot_ref,
    pixels_ref,
    table_ref,
    gain_one_ref,
    qkv_ref,
    proj_ref,
    gain_two_ref,
    hidden_ref,
    output_ref,
    restored_ref,
    work_ref,
    flat,
    mixed,
    natural,
    packed,
    bias,
    qkv_t,
    proj_t,
    hidden_t,
    gains,
    halo_out,
    halo_in,
    rows_out,
    rows_in,
    y_out,
    x_out,
    x_in,
    z_out,
    z_in,
    total_ref,
    done_ref,
    rows_sem,
    y_sem,
    x_sem,
    z_sem,
):
    me = lax.axis_index("band")
    bands = lax.axis_size("band")
    x = me // (Z_SIZE * Y_SIZE)
    z = lax.rem(me // Y_SIZE, Z_SIZE)
    y = lax.rem(me, Y_SIZE)
    x_peers = [band_of(x + step, z, y) for step in range(1, X_SIZE)]
    y_peer = band_of(x, z, y + 1)
    z_peers = [band_of(x, z + 1, y), band_of(x, z + Z_SIZE - 1, y)]
    after = lax.rem(me + 1, bands)
    before = lax.rem(me + bands - 1, bands)
    barrier = pltpu.get_barrier_semaphore()
    greeted = x_peers + [y_peer] + z_peers + [after, before]
    for peer in greeted:
        pl.semaphore_signal(barrier, inc=1, device_id={"band": peer}, device_id_type=MESH)

    blocks = ROWS_PAD // 8
    tiles = packed.shape[0] - 1
    window_total = active_ref.shape[0]
    half = CAP // 2
    far = Z_SIZE // 2
    order = [far]
    for away in range(far - 1, 0, -1):
        order += [away, Z_SIZE - away]
    order += [0]

    def copy(source, target, sems, index, peer):
        return pltpu.make_async_remote_copy(
            src_ref=source,
            dst_ref=target,
            send_sem=sems.at[(0,) + index],
            recv_sem=sems.at[(1,) + index],
            device_id={"band": peer},
            device_id_type=MESH,
        )

    def halo_copy():
        return copy(halo_out, halo_in, rows_sem, (0,), before)

    def rows_copy():
        return copy(rows_out, rows_in, rows_sem, (1,), after)

    def y_copy(away):
        return copy(y_out.at[away], x_out.at[away, 1], y_sem, (away,), y_peer)

    def x_copy(away, ahead):
        return copy(
            x_out.at[away, :, ahead], x_in.at[away, ahead - 1], x_sem, (away, ahead - 1), x_peers[ahead - 1]
        )

    def z_copy(side, hop, part):
        piece = pl.ds(part * half, half)
        return copy(
            z_out.at[side, hop, piece], z_in.at[side, hop, piece], z_sem, (side, hop, part), z_peers[side]
        )

    group = 4

    def flatten(index, carry):
        values = pixels_ref[pl.ds(index * group, group)].astype(jnp.float32).reshape(group * WIN, 2 * LANES)
        at = pl.ds(pl.multiple_of(index * group * WIN, group * WIN), group * WIN)
        flat[0, at, :] = values[:, :LANES]
        flat[1, at, :] = values[:, LANES:]
        return carry

    lax.fori_loop(0, CHAN // group, flatten, 0, unroll=3)
    for part in range(2):
        flat[part, CHAN * WIN :, :] = jnp.zeros(((ROWS_PAD - CHAN) * WIN, LANES), jnp.float32)

    def row_block(part, block, row):
        return flat[part, pl.ds(block * 8 * WIN + row, 8, stride=WIN), :]

    def fill_halo(block, carry):
        at = pl.ds(pl.multiple_of(block * 8, 8), 8)
        for row in range(SHIFT):
            values = jnp.concatenate([row_block(0, block, row), row_block(1, block, row)], axis=1)
            halo_out[row, at, :] = values.astype(jnp.bfloat16)
        return carry

    lax.fori_loop(0, blocks, fill_halo, 0)
    pl.semaphore_wait(barrier, len(greeted))
    halo_copy().start()

    qkv_t[...] = lax.dot_general(
        head_columns(3 * HEADS), qkv_ref[...], (((1,), (1,)), ((), ())), preferred_element_type=jnp.float32
    ).astype(jnp.bfloat16)
    proj_t[...] = lax.dot_general(
        proj_ref[...], head_columns(HEADS), (((0,), (1,)), ((), ())), preferred_element_type=jnp.float32
    ).astype(jnp.bfloat16)
    hidden_t[...] = hidden_ref[...].astype(jnp.float32).T.astype(jnp.bfloat16)
    for index, gain_ref in enumerate((gain_one_ref, gain_two_ref)):
        gains[index] = jnp.broadcast_to(gain_ref[...], (LANES, CHAN)).T
    build_bias(table_ref, bias)
    source = iota((LANES, LANES), 0)
    target = iota((LANES, LANES), 1)

    def sorted_lane(lane):
        return ((lane >> 3) & (WIN - 1)) * (TILE * WIN) + (lane >> 6) * WIN + (lane & (WIN - 1))

    to_window = jnp.where(source == sorted_lane(target), 1.0, 0.0).astype(jnp.bfloat16)
    to_rows = jnp.where(target == sorted_lane(source), 1.0, 0.0).astype(jnp.bfloat16)

    halo_copy().wait_recv()

    def cut(block, carry):
        at = pl.ds(pl.multiple_of(block * 8, 8), 8)
        sides = [[], []]
        for row in range(WIN):
            if row < WIN - SHIFT:
                first, second = row_block(0, block, row + SHIFT), row_block(1, block, row + SHIFT)
            else:
                values = halo_in[row - WIN + SHIFT, at, :].astype(jnp.float32)
                first, second = values[:, :LANES], values[:, LANES:]
            first, second = shift_lanes(first, second, -SHIFT)
            sides[0].append(first)
            sides[1].append(second)
        for side in range(2):
            for index, values in enumerate(swap_blocks(sides[side])):
                mixed[side * 8 + index, at, :] = values
        return carry

    lax.fori_loop(0, blocks, cut, 0)

    def settle(tile, carry):
        natural[tile] = jnp.dot(
            mixed[tile].astype(jnp.bfloat16), to_window, preferred_element_type=jnp.float32
        )
        return carry

    lax.fori_loop(0, tiles, settle, 0, unroll=2)
    natural[tiles] = jnp.zeros((ROWS_PAD, LANES), jnp.float32)

    edge = CHAN - CHAN % 8
    edge_row = iota((ROWS_PAD - edge, LANES), 0) - (CHAN - edge)
    low = iota((ROWS_PAD, LANES), 1) < TOKENS
    low_edge = iota((ROWS_PAD - edge, LANES), 1) < TOKENS
    last_band = jnp.where(me == bands - 1, 1.0, 0.0)

    def finish_tile(values, slot, last_row, last_col):
        notes = jnp.where(edge_row == 0, slot, jnp.where(edge_row == 1, last_row, last_col))
        return jnp.concatenate(
            [values[:edge], jnp.where(edge_row < 0, values[edge:], notes)], axis=0
        ).astype(jnp.bfloat16)

    def pack(tile, carry):
        one = order_ref[tile * TILE]
        two = order_ref[tile * TILE + 1]
        first = natural[one >> 1]
        second = natural[two >> 1]
        first = jnp.where((one & 1) == 1, pltpu.roll(first, TOKENS, 1), first)
        second = jnp.where((two & 1) == 1, second, pltpu.roll(second, TOKENS, 1))
        last_col = jnp.where(
            low_edge,
            jnp.where(one == window_total - 1, 1.0, 0.0),
            jnp.where(two == window_total - 1, 1.0, 0.0),
        )
        packed[tile] = finish_tile(
            jnp.where(low, first, second), slot_ref[tile].astype(jnp.float32), last_band, last_col
        )
        return carry

    lax.fori_loop(0, tiles, pack, 0)
    packed[tiles] = finish_tile(natural[tiles], float(CAP), 0.0, 0.0)

    def stage(away):
        def step(ahead, carry):
            y_out[away, ahead] = packed[held_ref[band_of(x + ahead, z + away, y + 1)]]
            x_out[away, 0, ahead] = packed[held_ref[band_of(x + ahead, z + away, y)]]
            return carry

        lax.fori_loop(0, X_SIZE, step, 0)

    for away in order:
        stage(away)
        y_copy(away).start()

    def pass_x(away):
        y_copy(away).wait_recv()
        for ahead in range(1, X_SIZE):
            x_copy(away, ahead).start()

    def wait_x(away):
        for ahead in range(1, X_SIZE):
            x_copy(away, ahead).wait_recv()

    def gather(away, part, target, arrived):
        found = [x_out.at[away, 0, 0], x_out.at[away, 1, 0]]
        for ahead in range(X_SIZE - 1):
            found += [x_in.at[away, ahead, 0], x_in.at[away, ahead, 1]]

        def step(index, carry):
            slot = part * half + index
            number = slot.astype(jnp.float32)
            sum_ = None if arrived is None else arrived[slot]
            for one in found:
                mark = one[CHAN : CHAN + 1, :].astype(jnp.float32)
                term = one[...] * jnp.where(mark == number, 1.0, 0.0).astype(jnp.bfloat16)
                sum_ = term if sum_ is None else sum_ + term
            target[slot] = sum_
            return carry

        lax.fori_loop(0, half, step, 0)

    fed = [0]
    gaps = list(UNITS)

    def work(count=None):
        start = fed[0]
        count = tiles - start if count is None else min(count, tiles - start)
        if count == 0:
            return

        def step(tile, carry):
            values = natural[tile][:CHAN]
            last = jnp.logical_and(tile == tiles - 1, iota((TOKENS, LANES), 1) >= TOKENS)
            mask = region_mask(jnp.where(me == bands - 1, 1, 0), jnp.where(last, 1, 0))
            state = attend_tile(values, mask, gains[0], qkv_t[...], proj_t[...], bias)
            done = feed_tile(state, gains[1], hidden_t[...], output_ref[...])
            chosen = jnp.where(low[:CHAN], active_ref[tile * TILE], active_ref[tile * TILE + 1])
            done = jnp.where(chosen == 1, done, values).astype(jnp.bfloat16)
            mixed[tile, 0:CHAN, :] = jnp.dot(done, to_rows, preferred_element_type=jnp.float32)
            return carry

        lax.fori_loop(start, start + count, step, 0)
        fed[0] = start + count

    def fill():
        work(gaps.pop(0))

    def hop_far():
        wait_x(far)
        for side in range(2):
            gather(far, side, z_out.at[side, 0], None)
            z_copy(side, 0, side).start()

    def hop(side, number):
        away = far - number if side == 0 else Z_SIZE - far + number
        wait_x(away)
        parts = (1 - side, side) if number == 1 else (0, 1)
        for part in parts:
            if number == 1 and part != side:
                arrived = None
            else:
                z_copy(side, number - 1, part).wait_recv()
                arrived = z_in.at[side, number - 1]
            gather(away, part, z_out.at[side, number], arrived)
            z_copy(side, number, part).start()

    pass_x(order[0])
    fill()
    pass_x(order[1])
    fill()
    hop_far()
    pass_x(order[2])
    fill()
    pass_x(order[3])
    hop(0, 1)
    fill()
    hop(1, 1)
    pass_x(order[4])
    fill()
    pass_x(order[5])
    hop(0, 2)
    fill()
    hop(1, 2)
    pass_x(order[6])
    fill()
    pass_x(order[7])
    fill()
    hop(0, 3)
    fill()
    hop(1, 3)
    work()

    def join(block, carry):
        at = pl.ds(pl.multiple_of(block * 8, 8), 8)
        sides = [swap_blocks([mixed[side * 8 + index, at, :] for index in range(8)]) for side in range(2)]
        for row in range(WIN):
            first, second = shift_lanes(sides[0][row], sides[1][row], SHIFT)
            if row < WIN - SHIFT:
                place = pl.ds(block * 8 * WIN + row + SHIFT, 8, stride=WIN)
                flat[0, place, :] = first
                flat[1, place, :] = second
            else:
                values = jnp.concatenate([first, second], axis=1)
                rows_out[row - WIN + SHIFT, at, :] = values.astype(jnp.bfloat16)
        return carry

    lax.fori_loop(0, blocks, join, 0)
    rows_copy().start()
    wait_x(0)
    for part in range(2):
        gather(0, part, total_ref, None)
    for part in range(2):
        for side in range(2):
            z_copy(side, far - 1, part).wait_recv()

        def last_step(index, carry):
            slot = part * half + index
            values = total_ref[slot] + z_in[0, far - 1, slot] + z_in[1, far - 1, slot]
            values = values.astype(jnp.float32)
            last_row = values[CHAN + 1 : CHAN + 2]
            last_col = values[CHAN + 2 : CHAN + 3]
            mask = region_mask(jnp.where(last_row > 0, 1, 0), jnp.where(last_col > 0, 1, 0))
            state = attend_tile(values[:CHAN], mask, gains[0], qkv_t[...], proj_t[...], bias)
            done_ref[pl.ds(pl.multiple_of(slot * ROWS_PAD, 8), CHAN), :] = state.astype(jnp.float32)
            return carry

        lax.fori_loop(0, half, last_step, 0, unroll=2)

    def emit(index, carry):
        for inner in range(group):
            channel = index * group + inner
            work_ref[channel] = done_ref[pl.ds(channel, CAP, stride=ROWS_PAD), :].astype(jnp.bfloat16)
        return carry

    lax.fori_loop(0, CHAN // group, emit, 0)
    rows_copy().wait_recv()

    def take_rows(block, carry):
        at = pl.ds(pl.multiple_of(block * 8, 8), 8)
        for row in range(SHIFT):
            values = rows_in[row, at, :].astype(jnp.float32)
            place = pl.ds(block * 8 * WIN + row, 8, stride=WIN)
            flat[0, place, :] = values[:, :LANES]
            flat[1, place, :] = values[:, LANES:]
        return carry

    lax.fori_loop(0, blocks, take_rows, 0)

    def restore(index, carry):
        at = pl.ds(pl.multiple_of(index * group * WIN, group * WIN), group * WIN)
        values = jnp.concatenate([flat[0, at, :], flat[1, at, :]], axis=1)
        restored_ref[pl.ds(index * group, group)] = values.reshape(group, WIN, 2 * LANES).astype(jnp.bfloat16)
        return carry

    lax.fori_loop(0, CHAN // group, restore, 0, unroll=3)
    halo_copy().wait_send()
    rows_copy().wait_send()
    for away in order:
        y_copy(away).wait_send()
        for ahead in range(1, X_SIZE):
            x_copy(away, ahead).wait_send()
    for side in range(2):
        z_copy(side, 0, side).wait_send()
        for number in range(1, far):
            for part in range(2):
                z_copy(side, number, part).wait_send()


SMEM = pl.BlockSpec(memory_space=pltpu.SMEM)
VMEM = pl.BlockSpec(memory_space=pltpu.VMEM)


def shards(
    pixels,
    keep_mask,
    band_counts,
    plan_dest,
    plan_slot,
    bias_table,
    gain_attn,
    qkv_weight,
    proj_weight,
    gain_mlp,
    hidden_weight,
    output_weight,
):
    band_total = lax.axis_size("band")
    row_count, col_count, channels = pixels.shape
    window_total = keep_mask.shape[1]
    tile_total = window_total // TILE
    slots = plan_slot.reshape(-1)
    order, held, active = pl.pallas_call(
        plan_kernel,
        out_shape=[
            jax.ShapeDtypeStruct((window_total + 1,), jnp.int32),
            jax.ShapeDtypeStruct((band_total + 1,), jnp.int32),
            jax.ShapeDtypeStruct((window_total,), jnp.int32),
        ],
        in_specs=[SMEM] * 4,
        out_specs=[SMEM] * 3,
        name="plan",
    )(keep_mask.reshape(-1), band_counts, plan_dest.reshape(-1), slots)
    tile_shape = (ROWS_PAD, LANES)
    rows_shape = (SHIFT, ROWS_PAD, col_count)
    far = Z_SIZE // 2
    restored, work = pl.pallas_call(
        block_kernel,
        out_shape=[
            jax.ShapeDtypeStruct((channels, row_count, col_count), jnp.bfloat16),
            jax.ShapeDtypeStruct((channels, CAP, LANES), jnp.bfloat16),
        ],
        in_specs=[SMEM] * 4 + [VMEM] * 8,
        out_specs=[VMEM, VMEM],
        scratch_shapes=[
            pltpu.VMEM((2, ROWS_PAD * WIN, LANES), jnp.float32),
            pltpu.VMEM((tile_total,) + tile_shape, jnp.float32),
            pltpu.VMEM((tile_total + 1,) + tile_shape, jnp.float32),
            pltpu.VMEM((tile_total + 1,) + tile_shape, jnp.bfloat16),
            pltpu.VMEM((HEADS, TOKENS, LANES), jnp.float32),
            pltpu.VMEM((3 * HEADS * HEAD_PAD, CHAN), jnp.bfloat16),
            pltpu.VMEM((CHAN, HEADS * HEAD_PAD), jnp.bfloat16),
            pltpu.VMEM((FF_WIDTH, CHAN), jnp.bfloat16),
            pltpu.VMEM((2, CHAN, LANES), jnp.float32),
            pltpu.VMEM(rows_shape, jnp.bfloat16),
            pltpu.VMEM(rows_shape, jnp.bfloat16),
            pltpu.VMEM(rows_shape, jnp.bfloat16),
            pltpu.VMEM(rows_shape, jnp.bfloat16),
            pltpu.VMEM((Z_SIZE, X_SIZE) + tile_shape, jnp.bfloat16),
            pltpu.VMEM((Z_SIZE, Y_SIZE, X_SIZE) + tile_shape, jnp.bfloat16),
            pltpu.VMEM((Z_SIZE, X_SIZE - 1, Y_SIZE) + tile_shape, jnp.bfloat16),
            pltpu.VMEM((2, far, CAP) + tile_shape, jnp.bfloat16),
            pltpu.VMEM((2, far, CAP) + tile_shape, jnp.bfloat16),
            pltpu.VMEM((CAP,) + tile_shape, jnp.bfloat16),
            pltpu.VMEM((CAP * ROWS_PAD, LANES), jnp.float32),
            pltpu.SemaphoreType.DMA((2, 2)),
            pltpu.SemaphoreType.DMA((2, Z_SIZE)),
            pltpu.SemaphoreType.DMA((2, Z_SIZE, X_SIZE - 1)),
            pltpu.SemaphoreType.DMA((2, 2, far, 2)),
        ],
        compiler_params=pltpu.CompilerParams(
            vmem_limit_bytes=VMEM_LIMIT, collective_id=0, has_side_effects=True
        ),
        name="block",
    )(
        held,
        order,
        active,
        slots,
        jnp.transpose(pixels, (2, 0, 1)),
        bias_table.T,
        gain_attn.reshape(1, channels),
        qkv_weight,
        proj_weight,
        gain_mlp.reshape(1, channels),
        hidden_weight,
        output_weight.T,
    )
    return (jnp.transpose(restored, (1, 2, 0)), jnp.transpose(work, (1, 2, 0)))


def solution(mesh):
    sharded = P(("img", "band"))
    in_specs = (
        P(("img", "band"), None, None),
        P(("img", "band"), None),
        sharded,
        P(("img", "band"), None),
        P(("img", "band"), None),
    ) + (P(),) * 7
    out_specs = (P(("img", "band"), None, None), P(("img", "band"), None, None))
    return jax.shard_map(shards, mesh=mesh, in_specs=in_specs, out_specs=out_specs, check_vma=False)
```

```python
import jax
import jax.numpy as jnp
from jax import lax
from jax.experimental import pallas as pl
from jax.experimental.pallas import tpu as pltpu
from jax.sharding import PartitionSpec as P

CHAN = 180
FF_WIDTH = 360
HEADS = 6
HEAD_DIM = CHAN // HEADS
HEAD_PAD = 32
WIN = 8
TOKENS = WIN * WIN
TILE = 2
LANES = TILE * TOKENS
WIDE = 2 * LANES
SHIFT = 4
CAP = 8
ROWS_PAD = 184
X_SIZE = 4
Z_SIZE = 8
Y_SIZE = 2
EPSILON = 1e-05
MESH = pl.DeviceIdType.MESH
VMEM_LIMIT = 60 << 20


def iota(shape, dim):
    return lax.broadcasted_iota(jnp.int32, shape, dim)


def norm_columns(values, gain):
    center = values - jnp.sum(values, axis=0, keepdims=True) * (1.0 / CHAN)
    spread = jnp.sum(center * center, axis=0, keepdims=True) * (1.0 / CHAN)
    return (center * lax.rsqrt(spread + EPSILON) * gain).astype(jnp.bfloat16)


def split_two(values):
    high = values.astype(jnp.bfloat16)
    low = (values - high.astype(jnp.float32)).astype(jnp.bfloat16)
    return high, low


def attend_pair(x_cols, mask, gain, qkv_t, proj_t, bias_ref):
    low = (iota((TOKENS, WIDE), 1) & TOKENS) == 0
    low_head = (iota((HEAD_PAD, WIDE), 1) & TOKENS) == 0
    normed = norm_columns(x_cols, gain)
    qkv = jnp.dot(qkv_t, normed, preferred_element_type=jnp.float32)
    width = HEADS * HEAD_PAD
    none = jnp.zeros((3 * HEAD_PAD, LANES), jnp.bfloat16)
    mixed = []
    for head in range(HEADS):
        at = head * HEAD_PAD
        query = qkv[at : at + HEAD_PAD] * HEAD_DIM ** (-0.5)
        key = qkv[width + at : width + at + HEAD_PAD]
        value = qkv[2 * width + at : 2 * width + at + HEAD_PAD]
        query_high, query_low = split_two(query)
        key_high, key_low = split_two(key)
        left = jnp.concatenate([key_high, key_low, key_high], axis=0)
        left = jnp.concatenate([left[:, :LANES], left[:, LANES:]], axis=0)
        right = jnp.concatenate([query_high, query_high, query_low], axis=0)
        right = jnp.concatenate(
            [
                jnp.concatenate([right[:, :LANES], none], axis=1),
                jnp.concatenate([none, right[:, LANES:]], axis=1),
            ],
            axis=0,
        )
        full = lax.dot_general(
            left, right, (((0,), (0,)), ((), ())), preferred_element_type=jnp.float32
        )
        scores = jnp.where(low, full[:TOKENS], full[TOKENS:])
        line = bias_ref[head]
        scores = (scores + jnp.concatenate([line, line], axis=1)) + mask
        top = jnp.max(scores, axis=0, keepdims=True)
        grown = jnp.exp(scores - top)
        total = jnp.sum(grown, axis=0, keepdims=True)
        weights = (grown * (1.0 / total)).astype(jnp.bfloat16)
        parts = []
        for side in range(2):
            part = value[:, side * LANES : (side + 1) * LANES]
            parts += [part, pltpu.roll(part, TOKENS, 1)]
        values = jnp.concatenate(parts, axis=0).astype(jnp.bfloat16)[:, :TOKENS]
        sums = jnp.dot(values, weights, preferred_element_type=jnp.float32)
        sides = []
        for side in range(2):
            base = 2 * side * HEAD_PAD
            lanes = slice(side * LANES, (side + 1) * LANES)
            sides.append(
                jnp.where(
                    low_head[:, lanes],
                    sums[base : base + HEAD_PAD, lanes],
                    sums[base + HEAD_PAD : base + 2 * HEAD_PAD, lanes],
                )
            )
        mixed.append(jnp.concatenate(sides, axis=1).astype(jnp.bfloat16))
    mixed = jnp.concatenate(mixed, axis=0)
    projected = jnp.dot(proj_t, mixed, preferred_element_type=jnp.float32)
    return (x_cols + projected).astype(jnp.bfloat16)


def feed_pair(state, gain, hidden_t, output_t):
    state = state.astype(jnp.float32)
    normed = norm_columns(state, gain)
    hidden = jnp.dot(hidden_t, normed, preferred_element_type=jnp.float32)
    inner = jax.nn.gelu(hidden).astype(jnp.bfloat16)
    return state + jnp.dot(output_t, inner, preferred_element_type=jnp.float32)


def region_mask(rows_split, cols_split):
    key = iota((TOKENS, WIDE), 0)
    query = iota((TOKENS, WIDE), 1) & (TOKENS - 1)
    rows_differ = ((key ^ query) & (SHIFT * WIN)) != 0
    cols_differ = ((key ^ query) & SHIFT) != 0
    row_part = jnp.where(rows_differ, rows_split, 0)
    col_part = jnp.where(cols_differ, cols_split, 0)
    return jnp.where((row_part | col_part) != 0, -100.0, 0.0)


def head_columns(count):
    row = iota((count * HEAD_PAD, count * HEAD_DIM), 0)
    col = iota((count * HEAD_PAD, count * HEAD_DIM), 1)
    inside = row & (HEAD_PAD - 1)
    want = (row >> 5) * HEAD_DIM + inside
    hit = jnp.logical_and(inside < HEAD_DIM, col == want)
    return jnp.where(hit, 1.0, 0.0).astype(jnp.bfloat16)


def build_bias(table_ref, bias_ref):
    span = 2 * WIN - 1
    entries = table_ref.shape[1]
    entry = iota((entries, WIN * LANES), 0)
    lane = iota((entries, WIN * LANES), 1)
    key_col = lane >> 7
    place = lane & (LANES - 1)
    want = (place >> 3) * span + (place & (WIN - 1)) - key_col + WIN - 1
    onehot = jnp.where(entry == want, 1.0, 0.0)
    looked = jnp.dot(
        table_ref[...], onehot, precision=lax.Precision.HIGHEST, preferred_element_type=jnp.float32
    )
    low = iota((HEADS, LANES), 1) < TOKENS
    for col in range(WIN):
        line = looked[:, col * LANES : (col + 1) * LANES]
        for row in range(WIN):
            back = (WIN - 1 - row) * WIN
            moved = line if back == 0 else pltpu.roll(line, LANES - back, 1)
            moved = jnp.where(low, moved, pltpu.roll(moved, TOKENS, 1))
            bias_ref[:, row * WIN + col, :] = moved


def swap_blocks(blocks):
    lane = iota(blocks[0].shape, 1)
    blocks = list(blocks)
    for bit in range(3):
        width = 16 << bit
        low = (lane & width) == 0
        for one in range(8):
            if one & (1 << bit):
                continue
            two = one | (1 << bit)
            first, second = blocks[one], blocks[two]
            blocks[one] = jnp.where(low, first, pltpu.roll(second, width, 1))
            blocks[two] = jnp.where(low, pltpu.roll(first, LANES - width, 1), second)
    return blocks


def plan_kernel(keep_ref, count_ref, dest_ref, slot_ref, order_ref, held_ref, active_ref):
    total = active_ref.shape[0]
    bands = held_ref.shape[0] - 1
    tiles = dest_ref.shape[0]
    for place in range(total + 1):
        order_ref[place] = total
    for band in range(bands + 1):
        held_ref[band] = tiles

    def window_step(index, position):
        kept = keep_ref[index]
        live = jnp.logical_and(kept == 1, position < count_ref[0])
        order_ref[jnp.where(live, position, total)] = index
        active_ref[index] = live.astype(jnp.int32)
        return position + kept

    lax.fori_loop(0, total, window_step, jnp.int32(0))

    def tile_step(tile, carry):
        live = jnp.logical_and(tile * TILE < count_ref[0], slot_ref[tile] < CAP)
        held_ref[jnp.where(live, dest_ref[tile], bands)] = tile
        return carry

    lax.fori_loop(0, tiles, tile_step, 0)


def aligned(value):
    return value if isinstance(value, int) else pl.multiple_of(value, 8)


def band_of(x, z, y):
    return (lax.rem(x, X_SIZE) * Z_SIZE + lax.rem(z, Z_SIZE)) * Y_SIZE + lax.rem(y, Y_SIZE)


BLOCKS_AT_ONCE = 2
UNITS = (1, 0, 1, 1, 1, 1, 1, 1, 1)


def block_kernel(
    held_ref,
    order_ref,
    active_ref,
    slot_ref,
    pixels_ref,
    table_ref,
    gain_one_ref,
    qkv_ref,
    proj_ref,
    gain_two_ref,
    hidden_ref,
    output_ref,
    restored_ref,
    work_ref,
    flat,
    mixed,
    natural,
    packed,
    bias,
    qkv_t,
    proj_t,
    hidden_t,
    gains,
    halo_out,
    halo_in,
    rows_out,
    rows_in,
    y_out,
    x_out,
    x_in,
    z_out,
    z_in,
    total_ref,
    done_ref,
    rows_sem,
    y_sem,
    x_sem,
    z_sem,
):
    me = lax.axis_index("band")
    bands = lax.axis_size("band")
    x = me // (Z_SIZE * Y_SIZE)
    z = lax.rem(me // Y_SIZE, Z_SIZE)
    y = lax.rem(me, Y_SIZE)
    x_peers = [band_of(x + step, z, y) for step in range(1, X_SIZE)]
    y_peer = band_of(x, z, y + 1)
    z_peers = [band_of(x, z + 1, y), band_of(x, z + Z_SIZE - 1, y)]
    after = lax.rem(me + 1, bands)
    before = lax.rem(me + bands - 1, bands)
    barrier = pltpu.get_barrier_semaphore()
    greeted = x_peers + [y_peer] + z_peers + [after, before]
    for peer in greeted:
        pl.semaphore_signal(barrier, inc=1, device_id={"band": peer}, device_id_type=MESH)

    blocks = ROWS_PAD // 8
    tiles = packed.shape[0] - 1
    window_total = active_ref.shape[0]
    half = CAP // 2
    far = Z_SIZE // 2
    order = [far]
    for away in range(far - 1, 0, -1):
        order += [away, Z_SIZE - away]
    order += [0]

    def copy(source, target, sems, index, peer):
        return pltpu.make_async_remote_copy(
            src_ref=source,
            dst_ref=target,
            send_sem=sems.at[(0,) + index],
            recv_sem=sems.at[(1,) + index],
            device_id={"band": peer},
            device_id_type=MESH,
        )

    def halo_copy():
        return copy(halo_out, halo_in, rows_sem, (0,), before)

    def rows_copy():
        return copy(rows_out, rows_in, rows_sem, (1,), after)

    def y_copy(away):
        return copy(y_out.at[away], x_out.at[away, 1], y_sem, (away,), y_peer)

    def x_copy(away, ahead):
        return copy(
            x_out.at[away, :, ahead], x_in.at[away, ahead - 1], x_sem, (away, ahead - 1), x_peers[ahead - 1]
        )

    def z_copy(side, hop, part):
        piece = pl.ds(part * half, half)
        return copy(
            z_out.at[side, hop, piece], z_in.at[side, hop, piece], z_sem, (side, hop, part), z_peers[side]
        )

    group = 4

    def flatten(index, carry):
        values = pixels_ref[pl.ds(index * group, group)].astype(jnp.float32).reshape(group * WIN, 2 * LANES)
        at = pl.ds(pl.multiple_of(index * group * WIN, group * WIN), group * WIN)
        flat[0, at, :] = values[:, :LANES]
        flat[1, at, :] = values[:, LANES:]
        return carry

    lax.fori_loop(0, CHAN // group, flatten, 0, unroll=3)
    for part in range(2):
        flat[part, CHAN * WIN :, :] = jnp.zeros(((ROWS_PAD - CHAN) * WIN, LANES), jnp.float32)

    def row_block(part, block, row):
        return flat[part, pl.ds(block * 8 * WIN + row, 8, stride=WIN), :]

    def fill_halo(block, carry):
        at = pl.ds(pl.multiple_of(block * 8, 8), 8)
        for row in range(SHIFT):
            values = jnp.concatenate([row_block(0, block, row), row_block(1, block, row)], axis=1)
            halo_out[row, at, :] = values.astype(jnp.bfloat16)
        return carry

    lax.fori_loop(0, blocks, fill_halo, 0)
    pl.semaphore_wait(barrier, len(greeted))
    halo_copy().start()

    qkv_t[...] = lax.dot_general(
        head_columns(3 * HEADS), qkv_ref[...], (((1,), (1,)), ((), ())), preferred_element_type=jnp.float32
    ).astype(jnp.bfloat16)
    proj_t[...] = lax.dot_general(
        proj_ref[...], head_columns(HEADS), (((0,), (1,)), ((), ())), preferred_element_type=jnp.float32
    ).astype(jnp.bfloat16)
    hidden_t[...] = hidden_ref[...].astype(jnp.float32).T.astype(jnp.bfloat16)
    for index, gain_ref in enumerate((gain_one_ref, gain_two_ref)):
        gains[index] = jnp.broadcast_to(gain_ref[...], (LANES, CHAN)).T
    build_bias(table_ref, bias)
    source = iota((WIDE, LANES), 0)
    target = iota((WIDE, LANES), 1)
    place = (target >> 6) * WIN + (target & (WIN - 1)) + SHIFT
    found = ((target >> 3) & (WIN - 1)) * (TILE * WIN) + (place & 15) + (place >> 4) * LANES
    to_window = jnp.where(source == found, 1.0, 0.0).astype(jnp.bfloat16)
    place = ((target & 15) + TILE * WIN - SHIFT) & 15
    found = jnp.where((target & 15) < SHIFT, 0, LANES) + (place >> 3) * TOKENS
    found = found + (target >> 4) * WIN + (place & (WIN - 1))
    to_rows = jnp.where(source == found, 1.0, 0.0).astype(jnp.bfloat16)

    halo_copy().wait_recv()

    def cut(block, carry):
        at = pl.ds(aligned(block * 8), 8)
        sides = [[], []]
        for row in range(WIN):
            if row < WIN - SHIFT:
                first, second = row_block(0, block, row + SHIFT), row_block(1, block, row + SHIFT)
            else:
                values = halo_in[row - WIN + SHIFT, at, :].astype(jnp.float32)
                first, second = values[:, :LANES], values[:, LANES:]
            sides[0].append(first)
            sides[1].append(second)
        for side in range(2):
            for index, values in enumerate(swap_blocks(sides[side])):
                mixed[side * 8 + index, at, :] = values
        return carry

    def each_block(step):
        def body(index, carry):
            for inner in range(BLOCKS_AT_ONCE):
                step(index * BLOCKS_AT_ONCE + inner, 0)
            return carry

        whole = blocks // BLOCKS_AT_ONCE
        lax.fori_loop(0, whole, body, 0)
        for block in range(whole * BLOCKS_AT_ONCE, blocks):
            step(block, 0)

    each_block(cut)

    def settle(tile, carry):
        both = jnp.concatenate([mixed[tile], mixed[lax.rem(tile + 1, tiles)]], axis=1)
        natural[tile] = jnp.dot(
            both.astype(jnp.bfloat16), to_window, preferred_element_type=jnp.float32
        )
        return carry

    lax.fori_loop(0, tiles, settle, 0, unroll=2)
    natural[tiles] = jnp.zeros((ROWS_PAD, LANES), jnp.float32)

    edge = CHAN - CHAN % 8
    edge_row = iota((ROWS_PAD - edge, LANES), 0) - (CHAN - edge)
    low = iota((ROWS_PAD, LANES), 1) < TOKENS
    low_edge = iota((ROWS_PAD - edge, LANES), 1) < TOKENS
    last_band = jnp.where(me == bands - 1, 1.0, 0.0)

    def finish_tile(values, slot, last_row, last_col):
        notes = jnp.where(edge_row == 0, slot, jnp.where(edge_row == 1, last_row, last_col))
        return jnp.concatenate(
            [values[:edge], jnp.where(edge_row < 0, values[edge:], notes)], axis=0
        ).astype(jnp.bfloat16)

    def pack(tile, carry):
        one = order_ref[tile * TILE]
        two = order_ref[tile * TILE + 1]
        first = natural[one >> 1]
        second = natural[two >> 1]
        first = jnp.where((one & 1) == 1, pltpu.roll(first, TOKENS, 1), first)
        second = jnp.where((two & 1) == 1, second, pltpu.roll(second, TOKENS, 1))
        last_col = jnp.where(
            low_edge,
            jnp.where(one == window_total - 1, 1.0, 0.0),
            jnp.where(two == window_total - 1, 1.0, 0.0),
        )
        packed[tile] = finish_tile(
            jnp.where(low, first, second), slot_ref[tile].astype(jnp.float32), last_band, last_col
        )
        return carry

    lax.fori_loop(0, tiles, pack, 0)
    packed[tiles] = finish_tile(natural[tiles], float(CAP), 0.0, 0.0)

    def stage(away):
        def step(ahead, carry):
            y_out[away, ahead] = packed[held_ref[band_of(x + ahead, z + away, y + 1)]]
            x_out[away, 0, ahead] = packed[held_ref[band_of(x + ahead, z + away, y)]]
            return carry

        lax.fori_loop(0, X_SIZE, step, 0)

    for away in order:
        stage(away)
        y_copy(away).start()

    def pass_x(away):
        y_copy(away).wait_recv()
        for ahead in range(1, X_SIZE):
            x_copy(away, ahead).start()

    def wait_x(away):
        for ahead in range(1, X_SIZE):
            x_copy(away, ahead).wait_recv()

    def gather(away, part, target, arrived):
        found = [x_out.at[away, 0, 0], x_out.at[away, 1, 0]]
        for ahead in range(X_SIZE - 1):
            found += [x_in.at[away, ahead, 0], x_in.at[away, ahead, 1]]

        def step(index, carry):
            slot = part * half + index
            number = slot.astype(jnp.float32)
            sum_ = None if arrived is None else arrived[slot]
            for one in found:
                mark = one[CHAN : CHAN + 1, :].astype(jnp.float32)
                term = one[...] * jnp.where(mark == number, 1.0, 0.0).astype(jnp.bfloat16)
                sum_ = term if sum_ is None else sum_ + term
            target[slot] = sum_
            return carry

        lax.fori_loop(0, half, step, 0)

    fed = [0]
    gaps = list(UNITS)

    pairs = tiles // 2
    gain_one = jnp.concatenate([gains[0], gains[0]], axis=1)
    gain_two = jnp.concatenate([gains[1], gains[1]], axis=1)
    wide_low = iota((CHAN, LANES), 1) < TOKENS

    def work(count=None):
        start = fed[0]
        count = pairs - start if count is None else min(count, pairs - start)
        if count == 0:
            return

        def step(pair, carry):
            values = jnp.concatenate([natural[pair * 2][:CHAN], natural[pair * 2 + 1][:CHAN]], axis=1)
            last = jnp.logical_and(pair == pairs - 1, iota((TOKENS, WIDE), 1) >= WIDE - TOKENS)
            mask = region_mask(jnp.where(me == bands - 1, 1, 0), jnp.where(last, 1, 0))
            state = attend_pair(values, mask, gain_one, qkv_t[...], proj_t[...], bias)
            done = feed_pair(state, gain_two, hidden_t[...], output_ref[...])
            for side in range(2):
                tile = pair * 2 + side
                lanes = slice(side * LANES, (side + 1) * LANES)
                chosen = jnp.where(wide_low, active_ref[tile * TILE], active_ref[tile * TILE + 1])
                mixed[tile, 0:CHAN, :] = jnp.where(chosen == 1, done[:, lanes], values[:, lanes])
            return carry

        lax.fori_loop(start, start + count, step, 0)
        fed[0] = start + count

    def fill():
        work(gaps.pop(0))

    def hop_far():
        wait_x(far)
        for side in range(2):
            gather(far, side, z_out.at[side, 0], None)
            z_copy(side, 0, side).start()

    def hop(side, number):
        away = far - number if side == 0 else Z_SIZE - far + number
        wait_x(away)
        parts = (1 - side, side) if number == 1 else (0, 1)
        for part in parts:
            if number == 1 and part != side:
                arrived = None
            else:
                z_copy(side, number - 1, part).wait_recv()
                arrived = z_in.at[side, number - 1]
            gather(away, part, z_out.at[side, number], arrived)
            z_copy(side, number, part).start()

    pass_x(order[0])
    fill()
    pass_x(order[1])
    fill()
    hop_far()
    pass_x(order[2])
    fill()
    pass_x(order[3])
    hop(0, 1)
    fill()
    hop(1, 1)
    pass_x(order[4])
    fill()
    pass_x(order[5])
    hop(0, 2)
    fill()
    hop(1, 2)
    pass_x(order[6])
    fill()
    pass_x(order[7])
    fill()
    hop(0, 3)
    fill()
    hop(1, 3)
    work()

    def unsettle(tile, carry):
        both = jnp.concatenate([mixed[lax.rem(tile + tiles - 1, tiles)], mixed[tile]], axis=1)
        natural[tile] = jnp.dot(both.astype(jnp.bfloat16), to_rows, preferred_element_type=jnp.float32)
        return carry

    lax.fori_loop(0, tiles, unsettle, 0, unroll=2)

    def join(block, carry):
        at = pl.ds(aligned(block * 8), 8)
        sides = [swap_blocks([natural[side * 8 + index, at, :] for index in range(8)]) for side in range(2)]
        for row in range(WIN):
            first, second = sides[0][row], sides[1][row]
            if row < WIN - SHIFT:
                place = pl.ds(block * 8 * WIN + row + SHIFT, 8, stride=WIN)
                flat[0, place, :] = first
                flat[1, place, :] = second
            else:
                values = jnp.concatenate([first, second], axis=1)
                rows_out[row - WIN + SHIFT, at, :] = values.astype(jnp.bfloat16)
        return carry

    each_block(join)
    rows_copy().start()
    wait_x(0)
    for part in range(2):
        gather(0, part, total_ref, None)
    for part in range(2):
        for side in range(2):
            z_copy(side, far - 1, part).wait_recv()

        def last_step(index, carry):
            two = []
            for side in range(2):
                slot = part * half + index * 2 + side
                values = total_ref[slot] + z_in[0, far - 1, slot] + z_in[1, far - 1, slot]
                two.append(values.astype(jnp.float32))
            values = jnp.concatenate(two, axis=1)
            last_row = values[CHAN + 1 : CHAN + 2]
            last_col = values[CHAN + 2 : CHAN + 3]
            mask = region_mask(jnp.where(last_row > 0, 1, 0), jnp.where(last_col > 0, 1, 0))
            state = attend_pair(values[:CHAN], mask, gain_one, qkv_t[...], proj_t[...], bias)
            state = state.astype(jnp.float32)
            for side in range(2):
                slot = part * half + index * 2 + side
                lanes = slice(side * LANES, (side + 1) * LANES)
                done_ref[pl.ds(pl.multiple_of(slot * ROWS_PAD, 8), CHAN), :] = state[:, lanes]
            return carry

        lax.fori_loop(0, half // 2, last_step, 0)

    def emit(index, carry):
        for inner in range(group):
            channel = index * group + inner
            work_ref[channel] = done_ref[pl.ds(channel, CAP, stride=ROWS_PAD), :].astype(jnp.bfloat16)
        return carry

    lax.fori_loop(0, CHAN // group, emit, 0)
    rows_copy().wait_recv()

    def take_rows(block, carry):
        at = pl.ds(pl.multiple_of(block * 8, 8), 8)
        for row in range(SHIFT):
            values = rows_in[row, at, :].astype(jnp.float32)
            place = pl.ds(block * 8 * WIN + row, 8, stride=WIN)
            flat[0, place, :] = values[:, :LANES]
            flat[1, place, :] = values[:, LANES:]
        return carry

    lax.fori_loop(0, blocks, take_rows, 0)

    def restore(index, carry):
        at = pl.ds(pl.multiple_of(index * group * WIN, group * WIN), group * WIN)
        values = jnp.concatenate([flat[0, at, :], flat[1, at, :]], axis=1)
        restored_ref[pl.ds(index * group, group)] = values.reshape(group, WIN, 2 * LANES).astype(jnp.bfloat16)
        return carry

    lax.fori_loop(0, CHAN // group, restore, 0, unroll=3)
    halo_copy().wait_send()
    rows_copy().wait_send()
    for away in order:
        y_copy(away).wait_send()
        for ahead in range(1, X_SIZE):
            x_copy(away, ahead).wait_send()
    for side in range(2):
        z_copy(side, 0, side).wait_send()
        for number in range(1, far):
            for part in range(2):
                z_copy(side, number, part).wait_send()


SMEM = pl.BlockSpec(memory_space=pltpu.SMEM)
VMEM = pl.BlockSpec(memory_space=pltpu.VMEM)


def shards(
    pixels,
    keep_mask,
    band_counts,
    plan_dest,
    plan_slot,
    bias_table,
    gain_attn,
    qkv_weight,
    proj_weight,
    gain_mlp,
    hidden_weight,
    output_weight,
):
    band_total = lax.axis_size("band")
    row_count, col_count, channels = pixels.shape
    window_total = keep_mask.shape[1]
    tile_total = window_total // TILE
    slots = plan_slot.reshape(-1)
    order, held, active = pl.pallas_call(
        plan_kernel,
        out_shape=[
            jax.ShapeDtypeStruct((window_total + 1,), jnp.int32),
            jax.ShapeDtypeStruct((band_total + 1,), jnp.int32),
            jax.ShapeDtypeStruct((window_total,), jnp.int32),
        ],
        in_specs=[SMEM] * 4,
        out_specs=[SMEM] * 3,
        name="plan",
    )(keep_mask.reshape(-1), band_counts, plan_dest.reshape(-1), slots)
    tile_shape = (ROWS_PAD, LANES)
    rows_shape = (SHIFT, ROWS_PAD, col_count)
    far = Z_SIZE // 2
    restored, work = pl.pallas_call(
        block_kernel,
        out_shape=[
            jax.ShapeDtypeStruct((channels, row_count, col_count), jnp.bfloat16),
            jax.ShapeDtypeStruct((channels, CAP, LANES), jnp.bfloat16),
        ],
        in_specs=[SMEM] * 4 + [VMEM] * 8,
        out_specs=[VMEM, VMEM],
        scratch_shapes=[
            pltpu.VMEM((2, ROWS_PAD * WIN, LANES), jnp.float32),
            pltpu.VMEM((tile_total,) + tile_shape, jnp.float32),
            pltpu.VMEM((tile_total + 1,) + tile_shape, jnp.float32),
            pltpu.VMEM((tile_total + 1,) + tile_shape, jnp.bfloat16),
            pltpu.VMEM((HEADS, TOKENS, LANES), jnp.float32),
            pltpu.VMEM((3 * HEADS * HEAD_PAD, CHAN), jnp.bfloat16),
            pltpu.VMEM((CHAN, HEADS * HEAD_PAD), jnp.bfloat16),
            pltpu.VMEM((FF_WIDTH, CHAN), jnp.bfloat16),
            pltpu.VMEM((2, CHAN, LANES), jnp.float32),
            pltpu.VMEM(rows_shape, jnp.bfloat16),
            pltpu.VMEM(rows_shape, jnp.bfloat16),
            pltpu.VMEM(rows_shape, jnp.bfloat16),
            pltpu.VMEM(rows_shape, jnp.bfloat16),
            pltpu.VMEM((Z_SIZE, X_SIZE) + tile_shape, jnp.bfloat16),
            pltpu.VMEM((Z_SIZE, Y_SIZE, X_SIZE) + tile_shape, jnp.bfloat16),
            pltpu.VMEM((Z_SIZE, X_SIZE - 1, Y_SIZE) + tile_shape, jnp.bfloat16),
            pltpu.VMEM((2, far, CAP) + tile_shape, jnp.bfloat16),
            pltpu.VMEM((2, far, CAP) + tile_shape, jnp.bfloat16),
            pltpu.VMEM((CAP,) + tile_shape, jnp.bfloat16),
            pltpu.VMEM((CAP * ROWS_PAD, LANES), jnp.float32),
            pltpu.SemaphoreType.DMA((2, 2)),
            pltpu.SemaphoreType.DMA((2, Z_SIZE)),
            pltpu.SemaphoreType.DMA((2, Z_SIZE, X_SIZE - 1)),
            pltpu.SemaphoreType.DMA((2, 2, far, 2)),
        ],
        compiler_params=pltpu.CompilerParams(
            vmem_limit_bytes=VMEM_LIMIT, collective_id=0, has_side_effects=True
        ),
        name="block",
    )(
        held,
        order,
        active,
        slots,
        jnp.transpose(pixels, (2, 0, 1)),
        bias_table.T,
        gain_attn.reshape(1, channels),
        qkv_weight,
        proj_weight,
        gain_mlp.reshape(1, channels),
        hidden_weight,
        output_weight.T,
    )
    return (jnp.transpose(restored, (1, 2, 0)), jnp.transpose(work, (1, 2, 0)))


def solution(mesh):
    sharded = P(("img", "band"))
    in_specs = (
        P(("img", "band"), None, None),
        P(("img", "band"), None),
        sharded,
        P(("img", "band"), None),
        P(("img", "band"), None),
    ) + (P(),) * 7
    out_specs = (P(("img", "band"), None, None), P(("img", "band"), None, None))
    return jax.shard_map(shards, mesh=mesh, in_specs=in_specs, out_specs=out_specs, check_vma=False)
```

```python
import jax
import jax.numpy as jnp
from jax import lax
from jax.experimental import pallas as pl
from jax.experimental.pallas import tpu as pltpu
from jax.sharding import PartitionSpec as P

CHAN = 180
FF_WIDTH = 360
HEADS = 6
HEAD_DIM = CHAN // HEADS
HEAD_PAD = 32
WIN = 8
TOKENS = WIN * WIN
TILE = 2
LANES = TILE * TOKENS
WIDE = 2 * LANES
SHIFT = 4
CAP = 8
ROWS_PAD = 184
X_SIZE = 4
Z_SIZE = 8
Y_SIZE = 2
EPSILON = 1e-05
MESH = pl.DeviceIdType.MESH
VMEM_LIMIT = 60 << 20


def iota(shape, dim):
    return lax.broadcasted_iota(jnp.int32, shape, dim)


def norm_columns(values, gain):
    center = values - jnp.sum(values, axis=0, keepdims=True) * (1.0 / CHAN)
    spread = jnp.sum(center * center, axis=0, keepdims=True) * (1.0 / CHAN)
    return (center * lax.rsqrt(spread + EPSILON) * gain).astype(jnp.bfloat16)


def split_two(values):
    high = values.astype(jnp.bfloat16)
    low = (values - high.astype(jnp.float32)).astype(jnp.bfloat16)
    return high, low


def attend_pair(x_cols, mask, gain, qkv_t, proj_t, bias_ref):
    low = (iota((TOKENS, WIDE), 1) & TOKENS) == 0
    low_head = (iota((HEAD_PAD, WIDE), 1) & TOKENS) == 0
    normed = norm_columns(x_cols, gain)
    qkv = jnp.dot(qkv_t, normed, preferred_element_type=jnp.float32)
    width = HEADS * HEAD_PAD
    none = jnp.zeros((3 * HEAD_PAD, LANES), jnp.bfloat16)
    mixed = []
    for head in range(HEADS):
        at = head * HEAD_PAD
        query = qkv[at : at + HEAD_PAD] * HEAD_DIM ** (-0.5)
        key = qkv[width + at : width + at + HEAD_PAD]
        value = qkv[2 * width + at : 2 * width + at + HEAD_PAD]
        query_high, query_low = split_two(query)
        key_high, key_low = split_two(key)
        left = jnp.concatenate([key_high, key_low, key_high], axis=0)
        left = jnp.concatenate([left[:, :LANES], left[:, LANES:]], axis=0)
        right = jnp.concatenate([query_high, query_high, query_low], axis=0)
        right = jnp.concatenate(
            [
                jnp.concatenate([right[:, :LANES], none], axis=1),
                jnp.concatenate([none, right[:, LANES:]], axis=1),
            ],
            axis=0,
        )
        full = lax.dot_general(
            left, right, (((0,), (0,)), ((), ())), preferred_element_type=jnp.float32
        )
        scores = jnp.where(low, full[:TOKENS], full[TOKENS:])
        line = bias_ref[head]
        scores = (scores + jnp.concatenate([line, line], axis=1)) + mask
        top = jnp.max(scores, axis=0, keepdims=True)
        grown = jnp.exp(scores - top)
        total = jnp.sum(grown, axis=0, keepdims=True)
        weights = (grown * (1.0 / total)).astype(jnp.bfloat16)
        parts = []
        for side in range(2):
            part = value[:, side * LANES : (side + 1) * LANES]
            parts += [part, pltpu.roll(part, TOKENS, 1)]
        values = jnp.concatenate(parts, axis=0).astype(jnp.bfloat16)[:, :TOKENS]
        sums = jnp.dot(values, weights, preferred_element_type=jnp.float32)
        sides = []
        for side in range(2):
            base = 2 * side * HEAD_PAD
            lanes = slice(side * LANES, (side + 1) * LANES)
            sides.append(
                jnp.where(
                    low_head[:, lanes],
                    sums[base : base + HEAD_PAD, lanes],
                    sums[base + HEAD_PAD : base + 2 * HEAD_PAD, lanes],
                )
            )
        mixed.append(jnp.concatenate(sides, axis=1).astype(jnp.bfloat16))
    mixed = jnp.concatenate(mixed, axis=0)
    projected = jnp.dot(proj_t, mixed, preferred_element_type=jnp.float32)
    return (x_cols + projected).astype(jnp.bfloat16)


def feed_pair(state, gain, hidden_t, output_t):
    state = state.astype(jnp.float32)
    normed = norm_columns(state, gain)
    hidden = jnp.dot(hidden_t, normed, preferred_element_type=jnp.float32)
    inner = jax.nn.gelu(hidden).astype(jnp.bfloat16)
    return state + jnp.dot(output_t, inner, preferred_element_type=jnp.float32)


def region_mask(rows_split, cols_split):
    key = iota((TOKENS, WIDE), 0)
    query = iota((TOKENS, WIDE), 1) & (TOKENS - 1)
    rows_differ = ((key ^ query) & (SHIFT * WIN)) != 0
    cols_differ = ((key ^ query) & SHIFT) != 0
    row_part = jnp.where(rows_differ, rows_split, 0)
    col_part = jnp.where(cols_differ, cols_split, 0)
    return jnp.where((row_part | col_part) != 0, -100.0, 0.0)


def head_columns(count):
    row = iota((count * HEAD_PAD, count * HEAD_DIM), 0)
    col = iota((count * HEAD_PAD, count * HEAD_DIM), 1)
    inside = row & (HEAD_PAD - 1)
    want = (row >> 5) * HEAD_DIM + inside
    hit = jnp.logical_and(inside < HEAD_DIM, col == want)
    return jnp.where(hit, 1.0, 0.0).astype(jnp.bfloat16)


def build_bias(table_ref, bias_ref):
    span = 2 * WIN - 1
    entries = table_ref.shape[1]
    entry = iota((entries, WIN * LANES), 0)
    lane = iota((entries, WIN * LANES), 1)
    key_col = lane >> 7
    place = lane & (LANES - 1)
    want = (place >> 3) * span + (place & (WIN - 1)) - key_col + WIN - 1
    onehot = jnp.where(entry == want, 1.0, 0.0)
    looked = jnp.dot(
        table_ref[...], onehot, precision=lax.Precision.HIGHEST, preferred_element_type=jnp.float32
    )
    low = iota((HEADS, LANES), 1) < TOKENS
    for col in range(WIN):
        line = looked[:, col * LANES : (col + 1) * LANES]
        for row in range(WIN):
            back = (WIN - 1 - row) * WIN
            moved = line if back == 0 else pltpu.roll(line, LANES - back, 1)
            moved = jnp.where(low, moved, pltpu.roll(moved, TOKENS, 1))
            bias_ref[:, row * WIN + col, :] = moved


def swap_blocks(blocks):
    lane = iota(blocks[0].shape, 1)
    blocks = list(blocks)
    for bit in range(3):
        width = 16 << bit
        low = (lane & width) == 0
        for one in range(8):
            if one & (1 << bit):
                continue
            two = one | (1 << bit)
            first, second = blocks[one], blocks[two]
            blocks[one] = jnp.where(low, first, pltpu.roll(second, width, 1))
            blocks[two] = jnp.where(low, pltpu.roll(first, LANES - width, 1), second)
    return blocks


def hop_order():
    far = Z_SIZE // 2
    order = [far]
    for away in range(far - 1, 0, -1):
        order += [away, Z_SIZE - away]
    return order + [0]


def position():
    me = lax.axis_index("band")
    return me // (Z_SIZE * Y_SIZE), lax.rem(me // Y_SIZE, Z_SIZE), lax.rem(me, Y_SIZE)


def plan_kernel(keep_ref, count_ref, dest_ref, slot_ref, order_ref, held_ref, active_ref, list_ref, place_ref):
    total = active_ref.shape[0]
    bands = held_ref.shape[0] - 1
    tiles = dest_ref.shape[0]
    for place in range(total + 1):
        order_ref[place] = total
    for band in range(bands + 1):
        held_ref[band] = tiles

    def window_step(index, position):
        kept = keep_ref[index]
        live = jnp.logical_and(kept == 1, position < count_ref[0])
        order_ref[jnp.where(live, position, total)] = index
        active_ref[index] = live.astype(jnp.int32)
        return position + kept

    lax.fori_loop(0, total, window_step, jnp.int32(0))

    def tile_step(tile, carry):
        live = jnp.logical_and(tile * TILE < count_ref[0], slot_ref[tile] < CAP)
        held_ref[jnp.where(live, dest_ref[tile], bands)] = tile
        return carry

    lax.fori_loop(0, tiles, tile_step, 0)

    x, z, y = position()
    for index in range(tiles + 1):
        list_ref[index] = tiles
    count = jnp.int32(0)
    for away in hop_order():
        for ahead in range(X_SIZE):
            tile = held_ref[band_of(x + ahead, z + away, y + 1)]
            live = tile < tiles
            list_ref[jnp.where(live, count, tiles)] = tile
            place_ref[away * X_SIZE + ahead] = jnp.where(live, count, tiles)
            count = count + live.astype(jnp.int32)


def aligned(value):
    return value if isinstance(value, int) else pl.multiple_of(value, 8)


def band_of(x, z, y):
    return (lax.rem(x, X_SIZE) * Z_SIZE + lax.rem(z, Z_SIZE)) * Y_SIZE + lax.rem(y, Y_SIZE)


BLOCKS_AT_ONCE = 4
X_ORDER = (2, 1, 3)
OWN_FIRST = 3
UNITS = (2, 1, 1, 1, 1, 1, 1)


def block_kernel(
    held_ref,
    order_ref,
    active_ref,
    list_ref,
    slot_ref,
    place_ref,
    pixels_ref,
    table_ref,
    gain_one_ref,
    qkv_ref,
    proj_ref,
    gain_two_ref,
    hidden_ref,
    output_ref,
    restored_ref,
    work_ref,
    flat,
    mixed,
    natural,
    packed,
    bias,
    qkv_t,
    proj_t,
    hidden_t,
    gains,
    halo_out,
    halo_in,
    rows_out,
    rows_in,
    place_in,
    places,
    y_out,
    y_in_one,
    y_in_two,
    y_in_three,
    y_in_four,
    x_out,
    x_in,
    z_out,
    z_in,
    total_ref,
    done_ref,
    place_sem,
    halo_sem,
    rows_sem,
    y_sem,
    x_sem,
    z_sem,
):
    me = lax.axis_index("band")
    bands = lax.axis_size("band")
    x, z, y = position()
    x_peers = [band_of(x + step, z, y) for step in range(1, X_SIZE)]
    y_peer = band_of(x, z, y + 1)
    z_peers = [band_of(x, z + 1, y), band_of(x, z + Z_SIZE - 1, y)]
    after = lax.rem(me + 1, bands)
    before = lax.rem(me + bands - 1, bands)
    barrier = pltpu.get_barrier_semaphore()
    greeted = x_peers + [y_peer] + z_peers + [after, before]
    for peer in greeted:
        pl.semaphore_signal(barrier, inc=1, device_id={"band": peer}, device_id_type=MESH)

    blocks = ROWS_PAD // 8
    tiles = packed.shape[0] - 1
    window_total = active_ref.shape[0]
    half = CAP // 2
    far = Z_SIZE // 2
    order = hop_order()

    def copy(source, target, sems, index, peer):
        return pltpu.make_async_remote_copy(
            src_ref=source,
            dst_ref=target,
            send_sem=sems.at[(0,) + index],
            recv_sem=sems.at[(1,) + index],
            device_id={"band": peer},
            device_id_type=MESH,
        )

    def halo_copy(side):
        lanes = pl.ds(side * LANES, LANES)
        return copy(halo_out.at[:, :, lanes], halo_in.at[:, :, lanes], halo_sem, (side,), before)

    def rows_copy():
        return copy(rows_out, rows_in, rows_sem, (1,), after)

    y_ins = (y_in_one, y_in_two, y_in_three, y_in_four)
    y_piece = tiles // len(y_ins)

    def y_copy(index):
        piece = pl.ds(index * y_piece, y_piece)
        return copy(y_out.at[piece], y_ins[index].at[pl.ds(0, y_piece)], y_sem, (index,), y_peer)

    def place_copy():
        return copy(place_ref, place_in, rows_sem, (0,), y_peer)

    def x_copy(away, ahead, who):
        return copy(
            x_out.at[away, who, ahead],
            x_in.at[away, ahead - 1, who],
            x_sem,
            (away, ahead - 1, who),
            x_peers[ahead - 1],
        )

    def z_copy(side, hop, part):
        piece = pl.ds(part * half, half)
        return copy(
            z_out.at[side, hop, piece], z_in.at[side, hop, piece], z_sem, (side, hop, part), z_peers[side]
        )

    group = 4

    def flatten(index, carry):
        values = pixels_ref[pl.ds(index * group, group)].astype(jnp.float32).reshape(group * WIN, 2 * LANES)
        at = pl.ds(pl.multiple_of(index * group * WIN, group * WIN), group * WIN)
        flat[0, at, :] = values[:, :LANES]
        flat[1, at, :] = values[:, LANES:]
        return carry

    lax.fori_loop(0, CHAN // group, flatten, 0, unroll=3)
    for part in range(2):
        flat[part, CHAN * WIN :, :] = jnp.zeros(((ROWS_PAD - CHAN) * WIN, LANES), jnp.float32)

    def row_block(part, block, row):
        return flat[part, pl.ds(block * 8 * WIN + row, 8, stride=WIN), :]

    def fill_halo(block, carry):
        at = pl.ds(pl.multiple_of(block * 8, 8), 8)
        for row in range(SHIFT):
            values = jnp.concatenate([row_block(0, block, row), row_block(1, block, row)], axis=1)
            halo_out[row, at, :] = values.astype(jnp.bfloat16)
        return carry

    lax.fori_loop(0, blocks, fill_halo, 0)
    pl.semaphore_wait(barrier, len(greeted))
    place_copy().start()
    for side in range(2):
        halo_copy(side).start()

    qkv_t[...] = lax.dot_general(
        head_columns(3 * HEADS), qkv_ref[...], (((1,), (1,)), ((), ())), preferred_element_type=jnp.float32
    ).astype(jnp.bfloat16)
    proj_t[...] = lax.dot_general(
        proj_ref[...], head_columns(HEADS), (((0,), (1,)), ((), ())), preferred_element_type=jnp.float32
    ).astype(jnp.bfloat16)
    hidden_t[...] = hidden_ref[...].astype(jnp.float32).T.astype(jnp.bfloat16)
    for index, gain_ref in enumerate((gain_one_ref, gain_two_ref)):
        gains[index] = jnp.broadcast_to(gain_ref[...], (LANES, CHAN)).T
    build_bias(table_ref, bias)
    source = iota((WIDE, LANES), 0)
    target = iota((WIDE, LANES), 1)
    place = (target >> 6) * WIN + (target & (WIN - 1)) + SHIFT
    found = ((target >> 3) & (WIN - 1)) * (TILE * WIN) + (place & 15) + (place >> 4) * LANES
    to_window = jnp.where(source == found, 1.0, 0.0).astype(jnp.bfloat16)
    place = ((target & 15) + TILE * WIN - SHIFT) & 15
    found = jnp.where((target & 15) < SHIFT, 0, LANES) + (place >> 3) * TOKENS
    found = found + (target >> 4) * WIN + (place & (WIN - 1))
    to_rows = jnp.where(source == found, 1.0, 0.0).astype(jnp.bfloat16)

    def cut(side, block):
        at = pl.ds(aligned(block * 8), 8)
        lanes = slice(side * LANES, (side + 1) * LANES)
        lines = [row_block(side, block, row + SHIFT) for row in range(WIN - SHIFT)]
        lines += [halo_in[row, at, lanes].astype(jnp.float32) for row in range(SHIFT)]
        for index, values in enumerate(swap_blocks(lines)):
            mixed[side * 8 + index, at, :] = values

    def each_block(step):
        def body(index, carry):
            for inner in range(BLOCKS_AT_ONCE):
                step(index * BLOCKS_AT_ONCE + inner, 0)
            return carry

        whole = blocks // BLOCKS_AT_ONCE
        lax.fori_loop(0, whole, body, 0)
        for block in range(whole * BLOCKS_AT_ONCE, blocks):
            step(block, 0)

    for side in range(2):
        halo_copy(side).wait_recv()
        each_block(lambda block, carry, side=side: cut(side, block))

    def settle(tile, carry):
        both = jnp.concatenate([mixed[tile], mixed[lax.rem(tile + 1, tiles)]], axis=1)
        natural[tile] = jnp.dot(
            both.astype(jnp.bfloat16), to_window, preferred_element_type=jnp.float32
        )
        return carry

    lax.fori_loop(0, tiles, settle, 0, unroll=4)
    natural[tiles] = jnp.zeros((ROWS_PAD, LANES), jnp.float32)

    edge = CHAN - CHAN % 8
    edge_row = iota((ROWS_PAD - edge, LANES), 0) - (CHAN - edge)
    low = iota((ROWS_PAD, LANES), 1) < TOKENS
    low_edge = iota((ROWS_PAD - edge, LANES), 1) < TOKENS
    last_band = jnp.where(me == bands - 1, 1.0, 0.0)

    def finish_tile(values, slot, last_row, last_col):
        notes = jnp.where(edge_row == 0, slot, jnp.where(edge_row == 1, last_row, last_col))
        return jnp.concatenate(
            [values[:edge], jnp.where(edge_row < 0, values[edge:], notes)], axis=0
        ).astype(jnp.bfloat16)

    def pack(tile, carry):
        one = order_ref[tile * TILE]
        two = order_ref[tile * TILE + 1]
        first = natural[one >> 1]
        second = natural[two >> 1]
        first = jnp.where((one & 1) == 1, pltpu.roll(first, TOKENS, 1), first)
        second = jnp.where((two & 1) == 1, second, pltpu.roll(second, TOKENS, 1))
        last_col = jnp.where(
            low_edge,
            jnp.where(one == window_total - 1, 1.0, 0.0),
            jnp.where(two == window_total - 1, 1.0, 0.0),
        )
        packed[tile] = finish_tile(
            jnp.where(low, first, second), slot_ref[tile].astype(jnp.float32), last_band, last_col
        )
        return carry

    lax.fori_loop(0, tiles, pack, 0, unroll=2)
    packed[tiles] = finish_tile(natural[tiles], float(CAP), 0.0, 0.0)

    for y_in in y_ins:
        y_in[y_piece] = jnp.zeros((ROWS_PAD, LANES), jnp.bfloat16)

    def list_step(index, carry):
        y_out[index] = packed[list_ref[index]]
        return carry

    def own_x(away):
        def step(ahead, carry):
            x_out[away, 0, ahead] = packed[held_ref[band_of(x + ahead, z + away, y)]]
            return carry

        lax.fori_loop(0, X_SIZE, step, 0)
        for ahead in X_ORDER:
            x_copy(away, ahead, 0).start()

    for index in range(4):
        lax.fori_loop(index * y_piece, (index + 1) * y_piece, list_step, 0)
        y_copy(index).start()
        if index < OWN_FIRST:
            own_x(order[index])
    place_copy().wait_recv()
    kept = pltpu.make_async_copy(place_in, places, place_sem)
    kept.start()
    kept.wait()

    def pass_x(index):
        away = order[index]
        if index < 4:
            y_copy(index).wait_recv()

        def step(ahead, carry):
            place = places[away * X_SIZE + ahead]
            found = None
            for piece in range(min(index + 1, len(y_ins))):
                within = place - piece * y_piece
                hit = jnp.logical_and(within >= 0, within < y_piece)
                one = y_ins[piece][jnp.where(hit, within, y_piece)]
                found = one if found is None else found + one
            x_out[away, 1, ahead] = found
            return carry

        lax.fori_loop(0, X_SIZE, step, 0)
        for ahead in X_ORDER:
            x_copy(away, ahead, 1).start()
        if index + OWN_FIRST < len(order):
            own_x(order[index + OWN_FIRST])

    def wait_x(away):
        for ahead in X_ORDER:
            for who in range(Y_SIZE):
                x_copy(away, ahead, who).wait_recv()

    def gather(away, part, target, arrived):
        found = [x_out.at[away, 0, 0], x_out.at[away, 1, 0]]
        for ahead in range(X_SIZE - 1):
            found += [x_in.at[away, ahead, 0], x_in.at[away, ahead, 1]]

        def step(index, carry):
            slot = part * half + index
            number = slot.astype(jnp.float32)
            sum_ = None if arrived is None else arrived[slot]
            for one in found:
                mark = one[CHAN : CHAN + 1, :].astype(jnp.float32)
                term = one[...] * jnp.where(mark == number, 1.0, 0.0).astype(jnp.bfloat16)
                sum_ = term if sum_ is None else sum_ + term
            target[slot] = sum_
            return carry

        lax.fori_loop(0, half, step, 0)

    fed = [0]
    gaps = list(UNITS)

    pairs = tiles // 2
    gain_one = jnp.concatenate([gains[0], gains[0]], axis=1)
    gain_two = jnp.concatenate([gains[1], gains[1]], axis=1)
    wide_low = iota((CHAN, LANES), 1) < TOKENS

    def work(count=None):
        start = fed[0]
        count = pairs - start if count is None else min(count, pairs - start)
        if count == 0:
            return

        def step(pair, carry):
            values = jnp.concatenate([natural[pair * 2][:CHAN], natural[pair * 2 + 1][:CHAN]], axis=1)
            last = jnp.logical_and(pair == pairs - 1, iota((TOKENS, WIDE), 1) >= WIDE - TOKENS)
            mask = region_mask(jnp.where(me == bands - 1, 1, 0), jnp.where(last, 1, 0))
            state = attend_pair(values, mask, gain_one, qkv_t[...], proj_t[...], bias)
            done = feed_pair(state, gain_two, hidden_t[...], output_ref[...])
            for side in range(2):
                tile = pair * 2 + side
                lanes = slice(side * LANES, (side + 1) * LANES)
                chosen = jnp.where(wide_low, active_ref[tile * TILE], active_ref[tile * TILE + 1])
                mixed[tile, 0:CHAN, :] = jnp.where(chosen == 1, done[:, lanes], values[:, lanes])
            return carry

        lax.fori_loop(start, start + count, step, 0)
        fed[0] = start + count

    def fill():
        work(gaps.pop(0))

    def hop_far():
        wait_x(far)
        for side in range(2):
            gather(far, side, z_out.at[side, 0], None)
            z_copy(side, 0, side).start()

    def hop(side, number):
        away = far - number if side == 0 else Z_SIZE - far + number
        wait_x(away)
        parts = (1 - side, side) if number == 1 else (0, 1)
        for part in parts:
            if number == 1 and part != side:
                arrived = None
            else:
                z_copy(side, number - 1, part).wait_recv()
                arrived = z_in.at[side, number - 1]
            gather(away, part, z_out.at[side, number], arrived)
            z_copy(side, number, part).start()

    pass_x(0)
    fill()
    pass_x(1)
    fill()
    hop_far()
    pass_x(2)
    fill()
    pass_x(3)
    fill()
    hop(0, 1)
    fill()
    hop(1, 1)
    pass_x(4)
    fill()
    pass_x(5)
    hop(0, 2)
    fill()
    hop(1, 2)
    pass_x(6)
    work()
    pass_x(7)

    def unsettle(tile, carry):
        both = jnp.concatenate([mixed[lax.rem(tile + tiles - 1, tiles)], mixed[tile]], axis=1)
        natural[tile] = jnp.dot(both.astype(jnp.bfloat16), to_rows, preferred_element_type=jnp.float32)
        return carry

    lax.fori_loop(0, tiles, unsettle, 0, unroll=4)

    def join(block, carry):
        at = pl.ds(aligned(block * 8), 8)
        sides = [swap_blocks([natural[side * 8 + index, at, :] for index in range(8)]) for side in range(2)]
        for row in range(WIN):
            first, second = sides[0][row], sides[1][row]
            if row < WIN - SHIFT:
                place = pl.ds(block * 8 * WIN + row + SHIFT, 8, stride=WIN)
                flat[0, place, :] = first
                flat[1, place, :] = second
            else:
                values = jnp.concatenate([first, second], axis=1)
                rows_out[row - WIN + SHIFT, at, :] = values.astype(jnp.bfloat16)
        return carry

    each_block(join)
    rows_copy().start()
    hop(0, 3)
    hop(1, 3)
    wait_x(0)
    for part in range(2):
        gather(0, part, total_ref, None)
    rows_copy().wait_recv()

    def take_rows(block, carry):
        at = pl.ds(pl.multiple_of(block * 8, 8), 8)
        for row in range(SHIFT):
            values = rows_in[row, at, :].astype(jnp.float32)
            place = pl.ds(block * 8 * WIN + row, 8, stride=WIN)
            flat[0, place, :] = values[:, :LANES]
            flat[1, place, :] = values[:, LANES:]
        return carry

    lax.fori_loop(0, blocks, take_rows, 0)

    def restore(index, carry):
        at = pl.ds(pl.multiple_of(index * group * WIN, group * WIN), group * WIN)
        values = jnp.concatenate([flat[0, at, :], flat[1, at, :]], axis=1)
        restored_ref[pl.ds(index * group, group)] = values.reshape(group, WIN, 2 * LANES).astype(jnp.bfloat16)
        return carry

    lax.fori_loop(0, CHAN // group, restore, 0, unroll=3)
    for part in range(2):
        for side in range(2):
            z_copy(side, far - 1, part).wait_recv()

        def last_step(index, carry):
            two = []
            for side in range(2):
                slot = part * half + index * 2 + side
                values = total_ref[slot] + z_in[0, far - 1, slot] + z_in[1, far - 1, slot]
                two.append(values.astype(jnp.float32))
            values = jnp.concatenate(two, axis=1)
            last_row = values[CHAN + 1 : CHAN + 2]
            last_col = values[CHAN + 2 : CHAN + 3]
            mask = region_mask(jnp.where(last_row > 0, 1, 0), jnp.where(last_col > 0, 1, 0))
            state = attend_pair(values[:CHAN], mask, gain_one, qkv_t[...], proj_t[...], bias)
            state = state.astype(jnp.float32)
            for side in range(2):
                slot = part * half + index * 2 + side
                lanes = slice(side * LANES, (side + 1) * LANES)
                done_ref[pl.ds(pl.multiple_of(slot * ROWS_PAD, 8), CHAN), :] = state[:, lanes]
            return carry

        lax.fori_loop(0, half // 2, last_step, 0)

    def emit(index, carry):
        for inner in range(group):
            channel = index * group + inner
            work_ref[channel] = done_ref[pl.ds(channel, CAP, stride=ROWS_PAD), :].astype(jnp.bfloat16)
        return carry

    lax.fori_loop(0, CHAN // group, emit, 0)
    for side in range(2):
        halo_copy(side).wait_send()
    rows_copy().wait_send()
    place_copy().wait_send()
    for index in range(4):
        y_copy(index).wait_send()
    for away in order:
        for ahead in X_ORDER:
            for who in range(Y_SIZE):
                x_copy(away, ahead, who).wait_send()
    for side in range(2):
        z_copy(side, 0, side).wait_send()
        for number in range(1, far):
            for part in range(2):
                z_copy(side, number, part).wait_send()


SMEM = pl.BlockSpec(memory_space=pltpu.SMEM)
VMEM = pl.BlockSpec(memory_space=pltpu.VMEM)


def shards(
    pixels,
    keep_mask,
    band_counts,
    plan_dest,
    plan_slot,
    bias_table,
    gain_attn,
    qkv_weight,
    proj_weight,
    gain_mlp,
    hidden_weight,
    output_weight,
):
    band_total = lax.axis_size("band")
    row_count, col_count, channels = pixels.shape
    window_total = keep_mask.shape[1]
    tile_total = window_total // TILE
    slots = plan_slot.reshape(-1)
    order, held, active, listed, place = pl.pallas_call(
        plan_kernel,
        out_shape=[
            jax.ShapeDtypeStruct((window_total + 1,), jnp.int32),
            jax.ShapeDtypeStruct((band_total + 1,), jnp.int32),
            jax.ShapeDtypeStruct((window_total,), jnp.int32),
            jax.ShapeDtypeStruct((tile_total + 1,), jnp.int32),
            jax.ShapeDtypeStruct((LANES,), jnp.int32),
        ],
        in_specs=[SMEM] * 4,
        out_specs=[SMEM] * 5,
        name="plan",
    )(keep_mask.reshape(-1), band_counts, plan_dest.reshape(-1), slots)
    tile_shape = (ROWS_PAD, LANES)
    rows_shape = (SHIFT, ROWS_PAD, col_count)
    far = Z_SIZE // 2
    restored, work = pl.pallas_call(
        block_kernel,
        out_shape=[
            jax.ShapeDtypeStruct((channels, row_count, col_count), jnp.bfloat16),
            jax.ShapeDtypeStruct((channels, CAP, LANES), jnp.bfloat16),
        ],
        in_specs=[SMEM] * 5 + [VMEM] * 9,
        out_specs=[VMEM, VMEM],
        scratch_shapes=[
            pltpu.VMEM((2, ROWS_PAD * WIN, LANES), jnp.float32),
            pltpu.VMEM((tile_total,) + tile_shape, jnp.float32),
            pltpu.VMEM((tile_total + 1,) + tile_shape, jnp.float32),
            pltpu.VMEM((tile_total + 1,) + tile_shape, jnp.bfloat16),
            pltpu.VMEM((HEADS, TOKENS, LANES), jnp.float32),
            pltpu.VMEM((3 * HEADS * HEAD_PAD, CHAN), jnp.bfloat16),
            pltpu.VMEM((CHAN, HEADS * HEAD_PAD), jnp.bfloat16),
            pltpu.VMEM((FF_WIDTH, CHAN), jnp.bfloat16),
            pltpu.VMEM((2, CHAN, LANES), jnp.float32),
            pltpu.VMEM(rows_shape, jnp.bfloat16),
            pltpu.VMEM(rows_shape, jnp.bfloat16),
            pltpu.VMEM(rows_shape, jnp.bfloat16),
            pltpu.VMEM(rows_shape, jnp.bfloat16),
            pltpu.VMEM((LANES,), jnp.int32),
            pltpu.SMEM((LANES,), jnp.int32),
            pltpu.VMEM((tile_total,) + tile_shape, jnp.bfloat16),
            pltpu.VMEM((tile_total // 4 + 1,) + tile_shape, jnp.bfloat16),
            pltpu.VMEM((tile_total // 4 + 1,) + tile_shape, jnp.bfloat16),
            pltpu.VMEM((tile_total // 4 + 1,) + tile_shape, jnp.bfloat16),
            pltpu.VMEM((tile_total // 4 + 1,) + tile_shape, jnp.bfloat16),
            pltpu.VMEM((Z_SIZE, Y_SIZE, X_SIZE) + tile_shape, jnp.bfloat16),
            pltpu.VMEM((Z_SIZE, X_SIZE - 1, Y_SIZE) + tile_shape, jnp.bfloat16),
            pltpu.VMEM((2, far, CAP) + tile_shape, jnp.bfloat16),
            pltpu.VMEM((2, far, CAP) + tile_shape, jnp.bfloat16),
            pltpu.VMEM((CAP,) + tile_shape, jnp.bfloat16),
            pltpu.VMEM((CAP * ROWS_PAD, LANES), jnp.float32),
            pltpu.SemaphoreType.DMA(()),
            pltpu.SemaphoreType.DMA((2, 2)),
            pltpu.SemaphoreType.DMA((2, 2)),
            pltpu.SemaphoreType.DMA((2, 4)),
            pltpu.SemaphoreType.DMA((2, Z_SIZE, X_SIZE - 1, Y_SIZE)),
            pltpu.SemaphoreType.DMA((2, 2, far, 2)),
        ],
        compiler_params=pltpu.CompilerParams(
            vmem_limit_bytes=VMEM_LIMIT, collective_id=0, has_side_effects=True
        ),
        name="block",
    )(
        held,
        order,
        active,
        listed,
        slots,
        place,
        jnp.transpose(pixels, (2, 0, 1)),
        bias_table.T,
        gain_attn.reshape(1, channels),
        qkv_weight,
        proj_weight,
        gain_mlp.reshape(1, channels),
        hidden_weight,
        output_weight.T,
    )
    return (jnp.transpose(restored, (1, 2, 0)), jnp.transpose(work, (1, 2, 0)))


def solution(mesh):
    sharded = P(("img", "band"))
    in_specs = (
        P(("img", "band"), None, None),
        P(("img", "band"), None),
        sharded,
        P(("img", "band"), None),
        P(("img", "band"), None),
    ) + (P(),) * 7
    out_specs = (P(("img", "band"), None, None), P(("img", "band"), None, None))
    return jax.shard_map(shards, mesh=mesh, in_specs=in_specs, out_specs=out_specs, check_vma=False)
```

```python
import jax
import jax.numpy as jnp
from jax import lax
from jax.experimental import pallas as pl
from jax.experimental.pallas import tpu as pltpu
from jax.sharding import PartitionSpec as P

CHAN = 180
FF_WIDTH = 360
HEADS = 6
HEAD_DIM = CHAN // HEADS
HEAD_PAD = 32
WIN = 8
TOKENS = WIN * WIN
TILE = 2
LANES = TILE * TOKENS
WIDE = 2 * LANES
SHIFT = 4
CAP = 8
ROWS_PAD = 184
X_SIZE = 4
Z_SIZE = 8
Y_SIZE = 2
EPSILON = 1e-05
MESH = pl.DeviceIdType.MESH
VMEM_LIMIT = 60 << 20


def iota(shape, dim):
    return lax.broadcasted_iota(jnp.int32, shape, dim)


def norm_columns(values, gain):
    center = values - jnp.sum(values, axis=0, keepdims=True) * (1.0 / CHAN)
    spread = jnp.sum(center * center, axis=0, keepdims=True) * (1.0 / CHAN)
    return (center * lax.rsqrt(spread + EPSILON) * gain).astype(jnp.bfloat16)


def split_two(values):
    high = values.astype(jnp.bfloat16)
    low = (values - high.astype(jnp.float32)).astype(jnp.bfloat16)
    return high, low


def attend_pair(x_cols, mask, gain, qkv_t, proj_t, bias_ref):
    low = (iota((TOKENS, WIDE), 1) & TOKENS) == 0
    low_head = (iota((HEAD_PAD, WIDE), 1) & TOKENS) == 0
    normed = norm_columns(x_cols, gain)
    qkv = jnp.dot(qkv_t, normed, preferred_element_type=jnp.float32)
    width = HEADS * HEAD_PAD
    none = jnp.zeros((3 * HEAD_PAD, LANES), jnp.bfloat16)
    mixed = []
    for head in range(HEADS):
        at = head * HEAD_PAD
        query = qkv[at : at + HEAD_PAD] * HEAD_DIM ** (-0.5)
        key = qkv[width + at : width + at + HEAD_PAD]
        value = qkv[2 * width + at : 2 * width + at + HEAD_PAD]
        query_high, query_low = split_two(query)
        key_high, key_low = split_two(key)
        left = jnp.concatenate([key_high, key_low, key_high], axis=0)
        left = jnp.concatenate([left[:, :LANES], left[:, LANES:]], axis=0)
        right = jnp.concatenate([query_high, query_high, query_low], axis=0)
        right = jnp.concatenate(
            [
                jnp.concatenate([right[:, :LANES], none], axis=1),
                jnp.concatenate([none, right[:, LANES:]], axis=1),
            ],
            axis=0,
        )
        full = lax.dot_general(
            left, right, (((0,), (0,)), ((), ())), preferred_element_type=jnp.float32
        )
        scores = jnp.where(low, full[:TOKENS], full[TOKENS:])
        line = bias_ref[head]
        scores = (scores + jnp.concatenate([line, line], axis=1)) + mask
        top = jnp.max(scores, axis=0, keepdims=True)
        grown = jnp.exp(scores - top)
        total = jnp.sum(grown, axis=0, keepdims=True)
        weights = (grown * (1.0 / total)).astype(jnp.bfloat16)
        parts = []
        for side in range(2):
            part = value[:, side * LANES : (side + 1) * LANES]
            parts += [part, pltpu.roll(part, TOKENS, 1)]
        values = jnp.concatenate(parts, axis=0).astype(jnp.bfloat16)[:, :TOKENS]
        sums = jnp.dot(values, weights, preferred_element_type=jnp.float32)
        sides = []
        for side in range(2):
            base = 2 * side * HEAD_PAD
            lanes = slice(side * LANES, (side + 1) * LANES)
            sides.append(
                jnp.where(
                    low_head[:, lanes],
                    sums[base : base + HEAD_PAD, lanes],
                    sums[base + HEAD_PAD : base + 2 * HEAD_PAD, lanes],
                )
            )
        mixed.append(jnp.concatenate(sides, axis=1).astype(jnp.bfloat16))
    mixed = jnp.concatenate(mixed, axis=0)
    projected = jnp.dot(proj_t, mixed, preferred_element_type=jnp.float32)
    return (x_cols + projected).astype(jnp.bfloat16)


def feed_pair(state, gain, hidden_t, output_t):
    state = state.astype(jnp.float32)
    normed = norm_columns(state, gain)
    hidden = jnp.dot(hidden_t, normed, preferred_element_type=jnp.float32)
    inner = jax.nn.gelu(hidden).astype(jnp.bfloat16)
    return state + jnp.dot(output_t, inner, preferred_element_type=jnp.float32)


def region_mask(rows_split, cols_split):
    key = iota((TOKENS, WIDE), 0)
    query = iota((TOKENS, WIDE), 1) & (TOKENS - 1)
    rows_differ = ((key ^ query) & (SHIFT * WIN)) != 0
    cols_differ = ((key ^ query) & SHIFT) != 0
    row_part = jnp.where(rows_differ, rows_split, 0)
    col_part = jnp.where(cols_differ, cols_split, 0)
    return jnp.where((row_part | col_part) != 0, -100.0, 0.0)


def head_columns(count):
    row = iota((count * HEAD_PAD, count * HEAD_DIM), 0)
    col = iota((count * HEAD_PAD, count * HEAD_DIM), 1)
    inside = row & (HEAD_PAD - 1)
    want = (row >> 5) * HEAD_DIM + inside
    hit = jnp.logical_and(inside < HEAD_DIM, col == want)
    return jnp.where(hit, 1.0, 0.0).astype(jnp.bfloat16)


def build_bias(table_ref, bias_ref):
    span = 2 * WIN - 1
    entries = table_ref.shape[1]
    entry = iota((entries, WIN * LANES), 0)
    lane = iota((entries, WIN * LANES), 1)
    key_col = lane >> 7
    place = lane & (LANES - 1)
    want = (place >> 3) * span + (place & (WIN - 1)) - key_col + WIN - 1
    onehot = jnp.where(entry == want, 1.0, 0.0)
    looked = jnp.dot(
        table_ref[...], onehot, precision=lax.Precision.HIGHEST, preferred_element_type=jnp.float32
    )
    low = iota((HEADS, LANES), 1) < TOKENS
    for col in range(WIN):
        line = looked[:, col * LANES : (col + 1) * LANES]
        for row in range(WIN):
            back = (WIN - 1 - row) * WIN
            moved = line if back == 0 else pltpu.roll(line, LANES - back, 1)
            moved = jnp.where(low, moved, pltpu.roll(moved, TOKENS, 1))
            bias_ref[:, row * WIN + col, :] = moved


def swap_blocks(blocks):
    lane = iota(blocks[0].shape, 1)
    blocks = list(blocks)
    for bit in range(3):
        width = 16 << bit
        low = (lane & width) == 0
        for one in range(8):
            if one & (1 << bit):
                continue
            two = one | (1 << bit)
            first, second = blocks[one], blocks[two]
            blocks[one] = jnp.where(low, first, pltpu.roll(second, width, 1))
            blocks[two] = jnp.where(low, pltpu.roll(first, LANES - width, 1), second)
    return blocks


def hop_order():
    far = Z_SIZE // 2
    order = [far]
    for away in range(far - 1, 0, -1):
        order += [away, Z_SIZE - away]
    return order + [0]


def position():
    me = lax.axis_index("band")
    return me // (Z_SIZE * Y_SIZE), lax.rem(me // Y_SIZE, Z_SIZE), lax.rem(me, Y_SIZE)


def plan_kernel(keep_ref, count_ref, dest_ref, slot_ref, order_ref, held_ref, active_ref, list_ref, place_ref):
    total = active_ref.shape[0]
    bands = held_ref.shape[0] - 1
    tiles = dest_ref.shape[0]
    for place in range(total + 1):
        order_ref[place] = total
    for band in range(bands + 1):
        held_ref[band] = tiles

    def window_step(index, position):
        kept = keep_ref[index]
        live = jnp.logical_and(kept == 1, position < count_ref[0])
        order_ref[jnp.where(live, position, total)] = index
        active_ref[index] = live.astype(jnp.int32)
        return position + kept

    lax.fori_loop(0, total, window_step, jnp.int32(0))

    def tile_step(tile, carry):
        live = jnp.logical_and(tile * TILE < count_ref[0], slot_ref[tile] < CAP)
        held_ref[jnp.where(live, dest_ref[tile], bands)] = tile
        return carry

    lax.fori_loop(0, tiles, tile_step, 0)

    x, z, y = position()
    for index in range(tiles + 1):
        list_ref[index] = tiles
    count = jnp.int32(0)
    for away in hop_order():
        for ahead in range(X_SIZE):
            tile = held_ref[band_of(x + ahead, z + away, y + 1)]
            live = tile < tiles
            list_ref[jnp.where(live, count, tiles)] = tile
            place_ref[away * X_SIZE + ahead] = jnp.where(live, count, tiles)
            count = count + live.astype(jnp.int32)


def aligned(value):
    return value if isinstance(value, int) else pl.multiple_of(value, 8)


def band_of(x, z, y):
    return (lax.rem(x, X_SIZE) * Z_SIZE + lax.rem(z, Z_SIZE)) * Y_SIZE + lax.rem(y, Y_SIZE)


BLOCKS_AT_ONCE = 4
X_ORDER = (2, 1, 3)
OWN_FIRST = 3
UNITS = (2, 1, 1, 1, 1, 1, 1)


def block_kernel(
    held_ref,
    order_ref,
    active_ref,
    list_ref,
    slot_ref,
    place_ref,
    pixels_ref,
    table_ref,
    gain_one_ref,
    qkv_ref,
    proj_ref,
    gain_two_ref,
    hidden_ref,
    output_ref,
    restored_ref,
    work_ref,
    flat,
    mixed,
    natural,
    packed,
    bias,
    qkv_t,
    proj_t,
    hidden_t,
    gains,
    halo_out,
    halo_in,
    rows_out,
    rows_in,
    place_in,
    places,
    y_out,
    y_in_one,
    y_in_two,
    y_in_three,
    y_in_four,
    x_out,
    x_in,
    z_out,
    z_in,
    total_ref,
    done_ref,
    place_sem,
    halo_sem,
    rows_sem,
    y_sem,
    x_sem,
    z_sem,
):
    me = lax.axis_index("band")
    bands = lax.axis_size("band")
    x, z, y = position()
    x_peers = [band_of(x + step, z, y) for step in range(1, X_SIZE)]
    y_peer = band_of(x, z, y + 1)
    z_peers = [band_of(x, z + 1, y), band_of(x, z + Z_SIZE - 1, y)]
    after = lax.rem(me + 1, bands)
    before = lax.rem(me + bands - 1, bands)
    barrier = pltpu.get_barrier_semaphore()
    greeted = x_peers + [y_peer] + z_peers + [after, before]
    for peer in greeted:
        pl.semaphore_signal(barrier, inc=1, device_id={"band": peer}, device_id_type=MESH)

    blocks = ROWS_PAD // 8
    tiles = packed.shape[0] - 1
    window_total = active_ref.shape[0]
    half = CAP // 2
    far = Z_SIZE // 2
    order = hop_order()

    def copy(source, target, sems, index, peer):
        return pltpu.make_async_remote_copy(
            src_ref=source,
            dst_ref=target,
            send_sem=sems.at[(0,) + index],
            recv_sem=sems.at[(1,) + index],
            device_id={"band": peer},
            device_id_type=MESH,
        )

    def halo_copy(side):
        lanes = pl.ds(side * LANES, LANES)
        return copy(halo_out.at[:, :, lanes], halo_in.at[:, :, lanes], halo_sem, (side,), before)

    def rows_copy():
        return copy(rows_out, rows_in, rows_sem, (1,), after)

    y_ins = (y_in_one, y_in_two, y_in_three, y_in_four)
    y_piece = tiles // len(y_ins)

    def y_copy(index):
        piece = pl.ds(index * y_piece, y_piece)
        return copy(y_out.at[piece], y_ins[index].at[pl.ds(0, y_piece)], y_sem, (index,), y_peer)

    def place_copy():
        return copy(place_ref, place_in, rows_sem, (0,), y_peer)

    def x_copy(away, ahead, who):
        return copy(
            x_out.at[away, who, ahead],
            x_in.at[away, ahead - 1, who],
            x_sem,
            (away, ahead - 1, who),
            x_peers[ahead - 1],
        )

    def z_copy(side, hop, part):
        piece = pl.ds(part * half, half)
        return copy(
            z_out.at[side, hop, piece], z_in.at[side, hop, piece], z_sem, (side, hop, part), z_peers[side]
        )

    group = 4

    def flatten(index, carry):
        values = pixels_ref[pl.ds(index * group, group)].astype(jnp.float32).reshape(group * WIN, 2 * LANES)
        at = pl.ds(pl.multiple_of(index * group * WIN, group * WIN), group * WIN)
        flat[0, at, :] = values[:, :LANES]
        flat[1, at, :] = values[:, LANES:]
        return carry

    lax.fori_loop(0, CHAN // group, flatten, 0, unroll=3)
    for part in range(2):
        flat[part, CHAN * WIN :, :] = jnp.zeros(((ROWS_PAD - CHAN) * WIN, LANES), jnp.float32)

    def row_block(part, block, row):
        return flat[part, pl.ds(block * 8 * WIN + row, 8, stride=WIN), :]

    def fill_halo(block, carry):
        at = pl.ds(pl.multiple_of(block * 8, 8), 8)
        for row in range(SHIFT):
            values = jnp.concatenate([row_block(0, block, row), row_block(1, block, row)], axis=1)
            halo_out[row, at, :] = values.astype(jnp.bfloat16)
        return carry

    lax.fori_loop(0, blocks, fill_halo, 0)
    pl.semaphore_wait(barrier, len(greeted))
    place_copy().start()
    for side in range(2):
        halo_copy(side).start()

    qkv_t[...] = lax.dot_general(
        head_columns(3 * HEADS), qkv_ref[...], (((1,), (1,)), ((), ())), preferred_element_type=jnp.float32
    ).astype(jnp.bfloat16)
    proj_t[...] = lax.dot_general(
        proj_ref[...], head_columns(HEADS), (((0,), (1,)), ((), ())), preferred_element_type=jnp.float32
    ).astype(jnp.bfloat16)
    hidden_t[...] = hidden_ref[...].astype(jnp.float32).T.astype(jnp.bfloat16)
    for index, gain_ref in enumerate((gain_one_ref, gain_two_ref)):
        gains[index] = jnp.broadcast_to(gain_ref[...], (LANES, CHAN)).T
    build_bias(table_ref, bias)
    source = iota((WIDE, LANES), 0)
    target = iota((WIDE, LANES), 1)
    place = (target >> 6) * WIN + (target & (WIN - 1)) + SHIFT
    found = ((target >> 3) & (WIN - 1)) * (TILE * WIN) + (place & 15) + (place >> 4) * LANES
    to_window = jnp.where(source == found, 1.0, 0.0).astype(jnp.bfloat16)
    place = ((target & 15) + TILE * WIN - SHIFT) & 15
    found = jnp.where((target & 15) < SHIFT, 0, LANES) + (place >> 3) * TOKENS
    found = found + (target >> 4) * WIN + (place & (WIN - 1))
    to_rows = jnp.where(source == found, 1.0, 0.0).astype(jnp.bfloat16)

    def cut(side, block):
        at = pl.ds(aligned(block * 8), 8)
        lanes = slice(side * LANES, (side + 1) * LANES)
        lines = [row_block(side, block, row + SHIFT) for row in range(WIN - SHIFT)]
        lines += [halo_in[row, at, lanes].astype(jnp.float32) for row in range(SHIFT)]
        for index, values in enumerate(swap_blocks(lines)):
            mixed[side * 8 + index, at, :] = values

    def each_block(step):
        def body(index, carry):
            for inner in range(BLOCKS_AT_ONCE):
                step(index * BLOCKS_AT_ONCE + inner, 0)
            return carry

        whole = blocks // BLOCKS_AT_ONCE
        lax.fori_loop(0, whole, body, 0)
        for block in range(whole * BLOCKS_AT_ONCE, blocks):
            step(block, 0)

    for side in range(2):
        halo_copy(side).wait_recv()
        each_block(lambda block, carry, side=side: cut(side, block))

    def settle(tile, carry):
        both = jnp.concatenate([mixed[tile], mixed[lax.rem(tile + 1, tiles)]], axis=1)
        natural[tile] = jnp.dot(
            both.astype(jnp.bfloat16), to_window, preferred_element_type=jnp.float32
        )
        return carry

    lax.fori_loop(0, tiles, settle, 0, unroll=4)
    natural[tiles] = jnp.zeros((ROWS_PAD, LANES), jnp.float32)

    edge = CHAN - CHAN % 8
    edge_row = iota((ROWS_PAD - edge, LANES), 0) - (CHAN - edge)
    low = iota((ROWS_PAD, LANES), 1) < TOKENS
    low_edge = iota((ROWS_PAD - edge, LANES), 1) < TOKENS
    last_band = jnp.where(me == bands - 1, 1.0, 0.0)

    def finish_tile(values, slot, last_row, last_col):
        notes = jnp.where(edge_row == 0, slot, jnp.where(edge_row == 1, last_row, last_col))
        return jnp.concatenate(
            [values[:edge], jnp.where(edge_row < 0, values[edge:], notes)], axis=0
        ).astype(jnp.bfloat16)

    def pack(tile, carry):
        one = order_ref[tile * TILE]
        two = order_ref[tile * TILE + 1]
        first = natural[one >> 1]
        second = natural[two >> 1]
        first = jnp.where((one & 1) == 1, pltpu.roll(first, TOKENS, 1), first)
        second = jnp.where((two & 1) == 1, second, pltpu.roll(second, TOKENS, 1))
        last_col = jnp.where(
            low_edge,
            jnp.where(one == window_total - 1, 1.0, 0.0),
            jnp.where(two == window_total - 1, 1.0, 0.0),
        )
        packed[tile] = finish_tile(
            jnp.where(low, first, second), slot_ref[tile].astype(jnp.float32), last_band, last_col
        )
        return carry

    lax.fori_loop(0, tiles, pack, 0, unroll=4)
    packed[tiles] = finish_tile(natural[tiles], float(CAP), 0.0, 0.0)

    for y_in in y_ins:
        y_in[y_piece] = jnp.zeros((ROWS_PAD, LANES), jnp.bfloat16)

    def list_step(index, carry):
        y_out[index] = packed[list_ref[index]]
        return carry

    def own_x(away):
        def step(ahead, carry):
            x_out[away, 0, ahead] = packed[held_ref[band_of(x + ahead, z + away, y)]]
            return carry

        lax.fori_loop(0, X_SIZE, step, 0)
        for ahead in X_ORDER:
            x_copy(away, ahead, 0).start()

    for index in range(4):
        lax.fori_loop(index * y_piece, (index + 1) * y_piece, list_step, 0)
        y_copy(index).start()
        if index < OWN_FIRST:
            own_x(order[index])
    place_copy().wait_recv()
    kept = pltpu.make_async_copy(place_in, places, place_sem)
    kept.start()
    kept.wait()

    def pass_x(index):
        away = order[index]
        if index < 4:
            y_copy(index).wait_recv()

        def step(ahead, carry):
            place = places[away * X_SIZE + ahead]
            found = None
            for piece in range(min(index + 1, len(y_ins))):
                within = place - piece * y_piece
                hit = jnp.logical_and(within >= 0, within < y_piece)
                one = y_ins[piece][jnp.where(hit, within, y_piece)]
                found = one if found is None else found + one
            x_out[away, 1, ahead] = found
            return carry

        lax.fori_loop(0, X_SIZE, step, 0)
        for ahead in X_ORDER:
            x_copy(away, ahead, 1).start()
        if index + OWN_FIRST < len(order):
            own_x(order[index + OWN_FIRST])

    def wait_x(away):
        for ahead in X_ORDER:
            for who in range(Y_SIZE):
                x_copy(away, ahead, who).wait_recv()

    def gather(away, part, target, arrived):
        found = [x_out.at[away, 0, 0], x_out.at[away, 1, 0]]
        for ahead in range(X_SIZE - 1):
            found += [x_in.at[away, ahead, 0], x_in.at[away, ahead, 1]]

        def step(index, carry):
            slot = part * half + index
            number = slot.astype(jnp.float32)
            sum_ = None if arrived is None else arrived[slot]
            for one in found:
                mark = one[CHAN : CHAN + 1, :].astype(jnp.float32)
                term = one[...] * jnp.where(mark == number, 1.0, 0.0).astype(jnp.bfloat16)
                sum_ = term if sum_ is None else sum_ + term
            target[slot] = sum_
            return carry

        lax.fori_loop(0, half, step, 0, unroll=2)

    fed = [0]
    gaps = list(UNITS)

    pairs = tiles // 2
    gain_one = jnp.concatenate([gains[0], gains[0]], axis=1)
    gain_two = jnp.concatenate([gains[1], gains[1]], axis=1)
    wide_low = iota((CHAN, LANES), 1) < TOKENS

    def work(count=None):
        start = fed[0]
        count = pairs - start if count is None else min(count, pairs - start)
        if count == 0:
            return

        def step(pair, carry):
            values = jnp.concatenate([natural[pair * 2][:CHAN], natural[pair * 2 + 1][:CHAN]], axis=1)
            last = jnp.logical_and(pair == pairs - 1, iota((TOKENS, WIDE), 1) >= WIDE - TOKENS)
            mask = region_mask(jnp.where(me == bands - 1, 1, 0), jnp.where(last, 1, 0))
            state = attend_pair(values, mask, gain_one, qkv_t[...], proj_t[...], bias)
            done = feed_pair(state, gain_two, hidden_t[...], output_ref[...])
            for side in range(2):
                tile = pair * 2 + side
                lanes = slice(side * LANES, (side + 1) * LANES)
                chosen = jnp.where(wide_low, active_ref[tile * TILE], active_ref[tile * TILE + 1])
                mixed[tile, 0:CHAN, :] = jnp.where(chosen == 1, done[:, lanes], values[:, lanes])
            return carry

        lax.fori_loop(start, start + count, step, 0)
        fed[0] = start + count

    def fill():
        work(gaps.pop(0))

    def hop_far():
        wait_x(far)
        for side in range(2):
            gather(far, side, z_out.at[side, 0], None)
            z_copy(side, 0, side).start()

    def hop(side, number):
        away = far - number if side == 0 else Z_SIZE - far + number
        wait_x(away)
        parts = (1 - side, side) if number == 1 else (0, 1)
        for part in parts:
            if number == 1 and part != side:
                arrived = None
            else:
                z_copy(side, number - 1, part).wait_recv()
                arrived = z_in.at[side, number - 1]
            gather(away, part, z_out.at[side, number], arrived)
            z_copy(side, number, part).start()

    pass_x(0)
    fill()
    pass_x(1)
    fill()
    hop_far()
    pass_x(2)
    fill()
    pass_x(3)
    fill()
    hop(0, 1)
    fill()
    hop(1, 1)
    pass_x(4)
    fill()
    pass_x(5)
    hop(0, 2)
    fill()
    hop(1, 2)
    pass_x(6)
    work()
    pass_x(7)

    def unsettle(tile, carry):
        both = jnp.concatenate([mixed[lax.rem(tile + tiles - 1, tiles)], mixed[tile]], axis=1)
        natural[tile] = jnp.dot(both.astype(jnp.bfloat16), to_rows, preferred_element_type=jnp.float32)
        return carry

    lax.fori_loop(0, tiles, unsettle, 0, unroll=4)

    def join(block, carry):
        at = pl.ds(aligned(block * 8), 8)
        sides = [swap_blocks([natural[side * 8 + index, at, :] for index in range(8)]) for side in range(2)]
        for row in range(WIN):
            first, second = sides[0][row], sides[1][row]
            if row < WIN - SHIFT:
                place = pl.ds(block * 8 * WIN + row + SHIFT, 8, stride=WIN)
                flat[0, place, :] = first
                flat[1, place, :] = second
            else:
                values = jnp.concatenate([first, second], axis=1)
                rows_out[row - WIN + SHIFT, at, :] = values.astype(jnp.bfloat16)
        return carry

    each_block(join)
    rows_copy().start()
    hop(0, 3)
    hop(1, 3)
    wait_x(0)
    for part in range(2):
        gather(0, part, total_ref, None)
    rows_copy().wait_recv()

    def take_rows(block, carry):
        at = pl.ds(pl.multiple_of(block * 8, 8), 8)
        for row in range(SHIFT):
            values = rows_in[row, at, :].astype(jnp.float32)
            place = pl.ds(block * 8 * WIN + row, 8, stride=WIN)
            flat[0, place, :] = values[:, :LANES]
            flat[1, place, :] = values[:, LANES:]
        return carry

    lax.fori_loop(0, blocks, take_rows, 0)

    def restore(index, carry):
        at = pl.ds(pl.multiple_of(index * group * WIN, group * WIN), group * WIN)
        values = jnp.concatenate([flat[0, at, :], flat[1, at, :]], axis=1)
        restored_ref[pl.ds(index * group, group)] = values.reshape(group, WIN, 2 * LANES).astype(jnp.bfloat16)
        return carry

    lax.fori_loop(0, CHAN // group, restore, 0, unroll=3)
    for part in range(2):
        for side in range(2):
            z_copy(side, far - 1, part).wait_recv()

        def last_step(index, carry):
            two = []
            for side in range(2):
                slot = part * half + index * 2 + side
                values = total_ref[slot] + z_in[0, far - 1, slot] + z_in[1, far - 1, slot]
                two.append(values.astype(jnp.float32))
            values = jnp.concatenate(two, axis=1)
            last_row = values[CHAN + 1 : CHAN + 2]
            last_col = values[CHAN + 2 : CHAN + 3]
            mask = region_mask(jnp.where(last_row > 0, 1, 0), jnp.where(last_col > 0, 1, 0))
            state = attend_pair(values[:CHAN], mask, gain_one, qkv_t[...], proj_t[...], bias)
            state = state.astype(jnp.float32)
            for side in range(2):
                slot = part * half + index * 2 + side
                lanes = slice(side * LANES, (side + 1) * LANES)
                done_ref[pl.ds(pl.multiple_of(slot * ROWS_PAD, 8), CHAN), :] = state[:, lanes]
            return carry

        lax.fori_loop(0, half // 2, last_step, 0, unroll=2)

    def emit(index, carry):
        for inner in range(group):
            channel = index * group + inner
            work_ref[channel] = done_ref[pl.ds(channel, CAP, stride=ROWS_PAD), :].astype(jnp.bfloat16)
        return carry

    lax.fori_loop(0, CHAN // group, emit, 0, unroll=3)
    for side in range(2):
        halo_copy(side).wait_send()
    rows_copy().wait_send()
    place_copy().wait_send()
    for index in range(4):
        y_copy(index).wait_send()
    for away in order:
        for ahead in X_ORDER:
            for who in range(Y_SIZE):
                x_copy(away, ahead, who).wait_send()
    for side in range(2):
        z_copy(side, 0, side).wait_send()
        for number in range(1, far):
            for part in range(2):
                z_copy(side, number, part).wait_send()


SMEM = pl.BlockSpec(memory_space=pltpu.SMEM)
VMEM = pl.BlockSpec(memory_space=pltpu.VMEM)


def shards(
    pixels,
    keep_mask,
    band_counts,
    plan_dest,
    plan_slot,
    bias_table,
    gain_attn,
    qkv_weight,
    proj_weight,
    gain_mlp,
    hidden_weight,
    output_weight,
):
    band_total = lax.axis_size("band")
    row_count, col_count, channels = pixels.shape
    window_total = keep_mask.shape[1]
    tile_total = window_total // TILE
    slots = plan_slot.reshape(-1)
    order, held, active, listed, place = pl.pallas_call(
        plan_kernel,
        out_shape=[
            jax.ShapeDtypeStruct((window_total + 1,), jnp.int32),
            jax.ShapeDtypeStruct((band_total + 1,), jnp.int32),
            jax.ShapeDtypeStruct((window_total,), jnp.int32),
            jax.ShapeDtypeStruct((tile_total + 1,), jnp.int32),
            jax.ShapeDtypeStruct((LANES,), jnp.int32),
        ],
        in_specs=[SMEM] * 4,
        out_specs=[SMEM] * 5,
        name="plan",
    )(keep_mask.reshape(-1), band_counts, plan_dest.reshape(-1), slots)
    tile_shape = (ROWS_PAD, LANES)
    rows_shape = (SHIFT, ROWS_PAD, col_count)
    far = Z_SIZE // 2
    restored, work = pl.pallas_call(
        block_kernel,
        out_shape=[
            jax.ShapeDtypeStruct((channels, row_count, col_count), jnp.bfloat16),
            jax.ShapeDtypeStruct((channels, CAP, LANES), jnp.bfloat16),
        ],
        in_specs=[SMEM] * 5 + [VMEM] * 9,
        out_specs=[VMEM, VMEM],
        scratch_shapes=[
            pltpu.VMEM((2, ROWS_PAD * WIN, LANES), jnp.float32),
            pltpu.VMEM((tile_total,) + tile_shape, jnp.float32),
            pltpu.VMEM((tile_total + 1,) + tile_shape, jnp.float32),
            pltpu.VMEM((tile_total + 1,) + tile_shape, jnp.bfloat16),
            pltpu.VMEM((HEADS, TOKENS, LANES), jnp.float32),
            pltpu.VMEM((3 * HEADS * HEAD_PAD, CHAN), jnp.bfloat16),
            pltpu.VMEM((CHAN, HEADS * HEAD_PAD), jnp.bfloat16),
            pltpu.VMEM((FF_WIDTH, CHAN), jnp.bfloat16),
            pltpu.VMEM((2, CHAN, LANES), jnp.float32),
            pltpu.VMEM(rows_shape, jnp.bfloat16),
            pltpu.VMEM(rows_shape, jnp.bfloat16),
            pltpu.VMEM(rows_shape, jnp.bfloat16),
            pltpu.VMEM(rows_shape, jnp.bfloat16),
            pltpu.VMEM((LANES,), jnp.int32),
            pltpu.SMEM((LANES,), jnp.int32),
            pltpu.VMEM((tile_total,) + tile_shape, jnp.bfloat16),
            pltpu.VMEM((tile_total // 4 + 1,) + tile_shape, jnp.bfloat16),
            pltpu.VMEM((tile_total // 4 + 1,) + tile_shape, jnp.bfloat16),
            pltpu.VMEM((tile_total // 4 + 1,) + tile_shape, jnp.bfloat16),
            pltpu.VMEM((tile_total // 4 + 1,) + tile_shape, jnp.bfloat16),
            pltpu.VMEM((Z_SIZE, Y_SIZE, X_SIZE) + tile_shape, jnp.bfloat16),
            pltpu.VMEM((Z_SIZE, X_SIZE - 1, Y_SIZE) + tile_shape, jnp.bfloat16),
            pltpu.VMEM((2, far, CAP) + tile_shape, jnp.bfloat16),
            pltpu.VMEM((2, far, CAP) + tile_shape, jnp.bfloat16),
            pltpu.VMEM((CAP,) + tile_shape, jnp.bfloat16),
            pltpu.VMEM((CAP * ROWS_PAD, LANES), jnp.float32),
            pltpu.SemaphoreType.DMA(()),
            pltpu.SemaphoreType.DMA((2, 2)),
            pltpu.SemaphoreType.DMA((2, 2)),
            pltpu.SemaphoreType.DMA((2, 4)),
            pltpu.SemaphoreType.DMA((2, Z_SIZE, X_SIZE - 1, Y_SIZE)),
            pltpu.SemaphoreType.DMA((2, 2, far, 2)),
        ],
        compiler_params=pltpu.CompilerParams(
            vmem_limit_bytes=VMEM_LIMIT, collective_id=0, has_side_effects=True
        ),
        name="block",
    )(
        held,
        order,
        active,
        listed,
        slots,
        place,
        jnp.transpose(pixels, (2, 0, 1)),
        bias_table.T,
        gain_attn.reshape(1, channels),
        qkv_weight,
        proj_weight,
        gain_mlp.reshape(1, channels),
        hidden_weight,
        output_weight.T,
    )
    return (jnp.transpose(restored, (1, 2, 0)), jnp.transpose(work, (1, 2, 0)))


def solution(mesh):
    sharded = P(("img", "band"))
    in_specs = (
        P(("img", "band"), None, None),
        P(("img", "band"), None),
        sharded,
        P(("img", "band"), None),
        P(("img", "band"), None),
    ) + (P(),) * 7
    out_specs = (P(("img", "band"), None, None), P(("img", "band"), None, None))
    return jax.shard_map(shards, mesh=mesh, in_specs=in_specs, out_specs=out_specs, check_vma=False)
```
